32 devices in a mesh: batch: 8 (over y, x, core), tensor: 4 (over z).
Axes of the slice: x: 2, y: 2, z: 4, core: 2. Of those that a mesh axis runs over, the one named last changes fastest.
Arguments:
- inputs: bfloat16 [8, 4096, 1024], P('batch'), may hold values from -6 to 6
- segments: int32 [8, 4096], P('batch'), may hold values from 0 to 7, never falling along the last dimension, each value on 1 to 2048 neighbouring positions
- valid: int32 [8, 4096], P('batch'), may hold values from 0 to 1, as said below
- w_query: bfloat16 [1024, 1024], P(None, 'tensor'), may hold values from -0.1875 to 0.1875
- b_query: bfloat16 [1024], P('tensor'), may hold values from -3 to 3
- w_key: bfloat16 [1024, 1024], P(None, 'tensor'), may hold values from -0.1875 to 0.1875
- w_value: bfloat16 [1024, 1024], P(None, 'tensor'), may hold values from -0.1875 to 0.1875
- b_value: bfloat16 [1024], P('tensor'), may hold values from -3 to 3
- w_out: bfloat16 [1024, 1024], P('tensor'), may hold values from -1.5 to 1.5
- b_out: bfloat16 [1024], P('tensor'), may hold values from -3 to 3
- gain_one: bfloat16 [1024], P('tensor'), may hold values from 0.25 to 1.75
- shift_one: bfloat16 [1024], P('tensor'), may hold values from -2 to 2
- w_up: bfloat16 [1024, 4096], P(None, 'tensor'), may hold values from -0.1875 to 0.1875
- b_up: bfloat16 [4096], P('tensor'), may hold values from -3 to 3
- w_down: bfloat16 [4096, 1024], P('tensor'), may hold values from -0.09375 to 0.09375
- b_down: bfloat16 [1024], P('tensor'), may hold values from -3 to 3
- gain_two: bfloat16 [1024], P('tensor'), may hold values from 0.25 to 1.75
- shift_two: bfloat16 [1024], P('tensor'), may hold values from -2 to 2
- lex_weight: bfloat16 [1024], P('tensor'), may hold values from -0.1875 to 0.1875
- lex_bias: bfloat16 [1], replicated, may hold values from -0.5 to 0.5
- cotangent: bfloat16 [8, 4096, 1024], P('batch', None, 'tensor'), may hold values from -6 to 6
Outputs:
- output: bfloat16 [8, 4096, 1024], P('batch', None, 'tensor')
- grad_inputs: bfloat16 [8, 4096, 1024], P('batch', None, 'tensor')
- grad_w_query: float32 [1024, 1024], P(None, 'tensor')
- grad_b_query: float32 [1024], P('tensor')
- grad_w_key: float32 [1024, 1024], P(None, 'tensor')
- grad_w_value: float32 [1024, 1024], P(None, 'tensor')
- grad_b_value: float32 [1024], P('tensor')
- grad_w_out: float32 [1024, 1024], P('tensor')
- grad_b_out: float32 [1024], P('tensor')
- grad_gain_one: float32 [1024], P('tensor')
- grad_shift_one: float32 [1024], P('tensor')
- grad_w_up: float32 [1024, 4096], P(None, 'tensor')
- grad_b_up: float32 [4096], P('tensor')
- grad_w_down: float32 [4096, 1024], P('tensor')
- grad_b_down: float32 [1024], P('tensor')
- grad_gain_two: float32 [1024], P('tensor')
- grad_shift_two: float32 [1024], P('tensor')
- lex_stats: float32 [2], replicated
The draws below stay inside these ranges and needn't reach their ends.
Inputs may be any that keep to these rules, and one draw needn't show every extreme that they name: `valid`: in each row, 1 on a leading run of tokens and 0 on the rest (its padding); at least a quarter of each row is 1.
All inputs are finite; a program needn't handle non-finite values.
Results may differ from the reference program's by a relative error of at most 0.02.
Values may be sent and summed in bfloat16 or wider, within the bound.
A program may use at most 256 MiB of HBM per device.

```python
import math
import jax
import jax.numpy as jnp
import numpy as np
from jax import lax

D = 1024
HEADS = 16
FF = 4096
HEAD_DIM = 64
ROW_LEN = 4096
ROWS = 8


def draw_valid(key, part):
    row_ids = jnp.arange(ROWS, dtype=jnp.int32)
    base_pad = 2 * ROW_LEN // 3 * (ROWS - 1 - row_ids) // max(ROWS - 1, 1)
    jitter = jax.random.randint(key, (ROWS,), 0, max(ROW_LEN // 16, 1), dtype=jnp.int32)
    padding = jnp.minimum(base_pad + jitter, ROW_LEN - ROW_LEN // 4)
    positions = jnp.arange(ROW_LEN, dtype=jnp.int32)
    return (positions[None, :] < (ROW_LEN - padding)[:, None]).astype(jnp.int32)


def levels(rng, dims, cuts, least, largest):
    def one(axis_at, blocks):
        heights = jax.random.uniform(jax.random.fold_in(jax.random.fold_in(rng, 6), axis_at), (blocks,), jnp.float32, least / len(cuts), largest / len(cuts))
        return jnp.repeat(jnp.exp(heights), dims[axis_at] // blocks).reshape((-1,) + (1,) * (len(dims) - axis_at - 1))

    level = one(*cuts[0])
    for cut in cuts[1:]:
        level = level * one(*cut)
    return level


def profile(count, total, reach, slope):
    loads = [(1 << 20) // math.isqrt(standing ** slope) + 1 for standing in range(2, count + 1)]
    spare, given = total - reach - (count - 1), [1] * (count - 1)
    while spare > 0:
        candidates = [i for i in range(count - 1) if given[i] < reach]
        whole, remaining = sum([loads[i] for i in candidates]), spare
        for i in candidates:
            addition = min(reach - given[i], max(1, remaining * loads[i] // whole), spare)
            given[i] = given[i] + addition
            spare = spare - addition
    return np.array([reach] + given)


def uneven_parts(rng, count, total, bound, skew):
    if count == 2:
        one = jax.random.randint(rng, (), max(1, total - bound), min(bound, total - 1) + 1)
        return jnp.stack([one, total - one])
    sizes = jnp.asarray(profile(count, total, bound, skew), jnp.int32)
    pairs = (count - 1) // 2
    giver, taker = sizes[1:1 + 2 * pairs:2], sizes[2:2 + 2 * pairs:2]
    room = jnp.minimum(giver - 1, bound - taker)
    passed = jax.random.randint(jax.random.fold_in(rng, 1), (pairs,), 0, 1 << 20) % (room + 1)
    sizes = sizes.at[1:1 + 2 * pairs:2].set(giver - passed).at[2:2 + 2 * pairs:2].set(taker + passed)
    return sizes[jax.random.permutation(jax.random.fold_in(rng, 2), count)]


def scatter_about(stream_key, extent, scale, limit, cuts=(), kind=jnp.bfloat16):
    loudness = levels(stream_key, extent, cuts, -0.22, 0.18) if cuts else 1.0
    values = jax.random.normal(stream_key, extent, jnp.float32) * scale * loudness
    return jnp.minimum(jnp.maximum(values, -limit), limit).astype(kind)


def setup_inputs(seed: int = 0) -> dict:
    splits = jax.random.split(jax.random.key(seed), 22)
    return {
        "inputs": scatter_about(splits[0], (ROWS, ROW_LEN, D), 1.0, 6.0, ((0, 8),)),
        "segments": jax.vmap(lambda own: jnp.searchsorted(jnp.cumsum(uneven_parts(own, max(4, ROW_LEN // 512), ROW_LEN, ROW_LEN // 2, 2)), jnp.arange(ROW_LEN), side="right"))(jax.random.split(splits[1], ROWS)).reshape((ROWS, ROW_LEN)).astype(jnp.int32),
        "valid": draw_valid(jax.random.fold_in(splits[21], 71), 0),
        "w_query": scatter_about(splits[3], (D, D), D ** -0.5, 0.1875, ((1, 4),)),
        "b_query": scatter_about(splits[4], (D,), 0.5, 3.0, ((0, 4),)),
        "w_key": scatter_about(splits[5], (D, D), D ** -0.5, 0.1875, ((1, 4),)),
        "w_value": scatter_about(splits[6], (D, D), D ** -0.5, 0.1875, ((1, 4),)),
        "b_value": scatter_about(splits[7], (D,), 0.5, 3.0, ((0, 4),)),
        "w_out": scatter_about(splits[8], (D, D), (D // 64) ** -0.5, 1.5, ((0, 4),)),
        "b_out": scatter_about(splits[9], (D,), 0.5, 3.0, ((0, 4),)),
        "gain_one": jnp.clip(1.0 + 0.15 * jax.random.normal(splits[10], (D,), jnp.float32), 0.25, 1.75).astype(jnp.bfloat16),
        "shift_one": scatter_about(splits[11], (D,), 0.3, 2.0, ((0, 4),)),
        "w_up": scatter_about(splits[12], (D, FF), D ** -0.5, 0.1875, ((1, 4),)),
        "b_up": scatter_about(splits[13], (FF,), 0.5, 3.0, ((0, 4),)),
        "w_down": scatter_about(splits[14], (FF, D), FF ** -0.5, 0.09375, ((0, 4),)),
        "b_down": scatter_about(splits[15], (D,), 0.5, 3.0, ((0, 4),)),
        "gain_two": jnp.clip(1.0 + 0.15 * jax.random.normal(splits[16], (D,), jnp.float32), 0.25, 1.75).astype(jnp.bfloat16),
        "shift_two": scatter_about(splits[17], (D,), 0.3, 2.0, ((0, 4),)),
        "lex_weight": scatter_about(splits[18], (D,), D ** -0.5, 0.1875, ((0, 4),)),
        "lex_bias": jnp.clip(jax.random.uniform(splits[19], (1,), jnp.float32, -0.5, 0.5), -0.5, 0.5).astype(jnp.bfloat16),
        "cotangent": scatter_about(splits[20], (ROWS, ROW_LEN, D), 1.0, 6.0, ((0, 8), (2, 4))),
    }


@jax.custom_vjp
def low(v):
    return lax.optimization_barrier(v.astype(jnp.bfloat16)).astype(jnp.float32)

@jax.custom_vjp
def low_back(v):
    return v

def low_keep(v):
    return (low(v), None)

def low_pass(kept, grad):
    return (grad,)

def back_keep(v):
    return (v, None)

def back_low(kept, grad):
    return (low(grad),)
low.defvjp(low_keep, low_pass)
low_back.defvjp(back_keep, back_low)
EPSILON = 1e-05
MASKED = -1e+30
PRECISE = lax.Precision.HIGHEST

def matmul(left, right):
    return jnp.dot(left, right, precision=PRECISE, preferred_element_type=jnp.float32)

def layer_norm(value, gain, shift):
    mean_value = lax.optimization_barrier(jnp.mean(value, axis=-1, keepdims=True))
    spread = lax.optimization_barrier(jnp.mean(value * value, axis=-1, keepdims=True)) - mean_value * mean_value
    return (value - mean_value) * lax.rsqrt(spread + EPSILON) * gain + shift

def gelu_exact(value):
    return 0.5 * value * (1.0 + lax.erf(value * (1.0 / math.sqrt(2.0))))

def attention_row(queries, key_rows, value_rows, seg_row, valid_row):
    seq_len = queries.shape[0]
    block_size = min(512, seq_len)
    score_scale = 1.0 / math.sqrt(HEAD_DIM)
    key_pos = jnp.arange(seq_len, dtype=jnp.int32)

    @jax.checkpoint
    def one_block(block_index):
        block_start = (block_index * block_size).astype(jnp.int32)
        query_block = lax.dynamic_slice_in_dim(queries, block_start, block_size, 0)
        seg_query = lax.dynamic_slice_in_dim(seg_row, block_start, block_size, 0)
        query_pos = block_start + jnp.arange(block_size, dtype=jnp.int32)
        allowed = (seg_query[:, None] == seg_row[None, :]) & (valid_row[None, :] == 1) | (query_pos[:, None] == key_pos[None, :])
        raw = low_back(jnp.einsum('qhd,khd->hqk', query_block, key_rows, precision=PRECISE) * score_scale)
        scores = jnp.where(allowed[None], raw, MASKED)
        row_max = lax.optimization_barrier(jnp.max(scores, axis=2, keepdims=True))
        expo = jnp.exp(scores - row_max)
        weights = low(expo / lax.optimization_barrier(jnp.sum(expo, axis=2, keepdims=True)))
        return jnp.einsum('hqk,khd->qhd', weights, value_rows, precision=PRECISE)
    blocks = lax.map(one_block, jnp.arange(seq_len // block_size, dtype=jnp.int32))
    return blocks.reshape(seq_len, HEADS * HEAD_DIM)

def row_forward(x_row, seg_row, valid_row, params):
    w_query, b_query, w_key, w_value, b_value, w_out, b_out, gain_one, shift_one, w_up, b_up, w_down, b_down, gain_two, shift_two = params
    seq_len = x_row.shape[0]
    queries = low_back(low(matmul(x_row, w_query) + b_query)).reshape(seq_len, HEADS, HEAD_DIM)
    key_rows = low_back(low(matmul(x_row, w_key))).reshape(seq_len, HEADS, HEAD_DIM)
    value_rows = low_back(low(matmul(x_row, w_value) + b_value)).reshape(seq_len, HEADS, HEAD_DIM)
    context = low_back(low(attention_row(queries, key_rows, value_rows, seg_row, valid_row)))
    attended = low_back(matmul(context, w_out))
    first = layer_norm(x_row + attended + b_out, gain_one, shift_one)
    pre_up = low_back(matmul(low(first), w_up) + b_up)
    hidden = low(gelu_exact(pre_up))
    branch = low_back(matmul(hidden, w_down))
    return layer_norm(first + branch + b_down, gain_two, shift_two)

def reference(inputs, segments, valid, w_query, b_query, w_key, w_value, b_value, w_out, b_out, gain_one, shift_one, w_up, b_up, w_down, b_down, gain_two, shift_two, lex_weight, lex_bias, cotangent):
    params = tuple((item.astype(jnp.float32) for item in (w_query, b_query, w_key, w_value, b_value, w_out, b_out, gain_one, shift_one, w_up, b_up, w_down, b_down, gain_two, shift_two)))
    x_all = inputs.astype(jnp.float32)
    checked_row = jax.checkpoint(row_forward)

    def whole(x_values, param_values):

        def scan_step(carried, row_items):
            x_row, seg_row, valid_row = row_items
            return (carried, checked_row(x_row, seg_row, valid_row, param_values))
        _, outputs = lax.scan(scan_step, jnp.zeros((), jnp.float32), (x_values, segments, valid))
        return outputs
    result, backward = jax.vjp(whole, x_all, params)
    grad_x, grad_params = backward(cotangent.astype(jnp.float32))
    lex_pre = jnp.einsum('rld,d->rl', result, lex_weight.astype(jnp.float32), precision=PRECISE) + lex_bias.astype(jnp.float32)[0]
    lex_values = jnp.maximum(lex_pre, 0.0)
    lex_above = jnp.where(lex_pre > 0.0, 1.0, 0.0).astype(jnp.float32)
    valid_float = valid.astype(jnp.float32)
    count_valid = jnp.sum(valid_float)
    lex_stats = jnp.stack([jnp.sum(lex_values * valid_float) / count_valid, jnp.sum(lex_above * valid_float) / count_valid])
    return (result.astype(jnp.bfloat16), grad_x.astype(jnp.bfloat16), grad_params[0], grad_params[1], grad_params[2], grad_params[3], grad_params[4], grad_params[5], grad_params[6], grad_params[7], grad_params[8], grad_params[9], grad_params[10], grad_params[11], grad_params[12], grad_params[13], grad_params[14], lex_stats)
```

```python
import math, functools
import jax
import jax.numpy as jnp
from jax import lax
from jax.experimental import pallas as pl
from jax.experimental.pallas import tpu as pltpu

HEAD_DIM = 64
MASKED = -1e30
NT = (((1,), (1,)), ((), ()))
NN = (((1,), (0,)), ((), ()))


def dot_f32(left, right, dims):
    return lax.dot_general(left, right, dims, preferred_element_type=jnp.float32)


def head_lanes(shape, slot):
    lane = lax.broadcasted_iota(jnp.int32, shape, 1)
    return (lane >= slot * HEAD_DIM) & (lane < (slot + 1) * HEAD_DIM)


def pick_head(block, head, pair_width):
    group, slot = divmod(head * HEAD_DIM, pair_width)
    pair = block[:, group * pair_width : (group + 1) * pair_width]
    if pair_width == HEAD_DIM:
        return pair
    return jnp.where(head_lanes(pair.shape, slot // HEAD_DIM), pair, jnp.zeros_like(pair))


def allowed_tile(key_start, query_start, low_row, high_row, size):
    key_pos = key_start + lax.broadcasted_iota(jnp.int32, (size, 1), 0)
    query_pos = query_start + lax.broadcasted_iota(jnp.int32, (1, size), 1)
    return ((key_pos >= low_row) & (key_pos < high_row)) | (key_pos == query_pos)


def forward_body(
    first_block, size, heads, pair_width,
    bounds_ref, q_ref, k_ref, vt_ref, low_ref, high_ref,
    ctx_ref, lse_ref,
    qh_ref, acc_ref, max_ref, sum_ref,
):
    block = first_block + pl.program_id(0)
    for head in range(heads):
        qh_ref[head] = pick_head(q_ref[...], head, pair_width) * jnp.bfloat16(0.125)
    acc_ref[...] = jnp.zeros_like(acc_ref)
    max_ref[...] = jnp.full_like(max_ref, MASKED)
    sum_ref[...] = jnp.zeros_like(sum_ref)
    low_first, low_last = bounds_ref[0, block], bounds_ref[1, block]
    high_first, high_last = bounds_ref[2, block], bounds_ref[3, block]
    lower = low_first // size
    count = jnp.maximum((high_last + size - 1) // size - lower, 0)
    extra = jnp.where(block < lower + count, 0, 1)

    def visit(key_block, masked):
        key_start = pl.multiple_of(key_block * size, size)
        keys = pl.ds(key_start, size)
        if masked:
            allowed = allowed_tile(
                key_start, block * size, low_ref[...], high_ref[...], size
            )
        for head in range(heads):
            base = head * HEAD_DIM // pair_width * pair_width
            scores = dot_f32(k_ref[keys, base : base + pair_width], qh_ref[head], NT)
            if masked:
                scores = jnp.where(allowed, scores, MASKED)
            old_max = max_ref[head]
            new_max = jnp.maximum(old_max, jnp.max(scores, axis=0, keepdims=True))
            expo = jnp.exp(scores - new_max)
            scale = jnp.exp(old_max - new_max)
            max_ref[head] = new_max
            sum_ref[head] = sum_ref[head] * scale + jnp.sum(expo, axis=0, keepdims=True)
            rows = slice(head * HEAD_DIM, (head + 1) * HEAD_DIM)
            acc_ref[rows, :] = acc_ref[rows, :] * scale + dot_f32(
                vt_ref[rows, keys], expo.astype(jnp.bfloat16), NN
            )

    def step(index, carry):
        key_block = jnp.where(index < count, lower + index, block)
        key_start = key_block * size
        full = (key_start >= low_last) & (key_start + size <= high_first)
        pl.when(full)(lambda: visit(key_block, False))
        pl.when(jnp.logical_not(full))(lambda: visit(key_block, True))
        return carry

    lax.fori_loop(0, count + extra, step, 0)
    for head in range(heads):
        rows = slice(head * HEAD_DIM, (head + 1) * HEAD_DIM)
        acc_ref[rows, :] = acc_ref[rows, :] / sum_ref[head]
        lse_ref[head : head + 1, :] = max_ref[head] + jnp.log(sum_ref[head])
    ctx_ref[...] = acc_ref[...].T.astype(jnp.bfloat16)


def block_size_of(tokens):
    return min(256, tokens)


def attend_forward(q, k, vt, low, high, bounds, first=0, last=None):
    tokens, width = q.shape
    size = block_size_of(tokens)
    heads = width // HEAD_DIM
    pair_width = min(128, width)
    last = tokens // size if last is None else last
    grid = last - first
    row_spec = pl.BlockSpec((1, size), lambda i, b: (0, i + first))
    return pl.pallas_call(
        functools.partial(forward_body, first, size, heads, pair_width),
        name="attend_forward",
        out_shape=(
            jax.ShapeDtypeStruct((grid * size, width), jnp.bfloat16),
            jax.ShapeDtypeStruct((heads, grid * size), jnp.float32),
        ),
        grid_spec=pltpu.PrefetchScalarGridSpec(
            num_scalar_prefetch=1,
            grid=(grid,),
            in_specs=[
                pl.BlockSpec((size, width), lambda i, b: (i + first, 0)),
                pl.BlockSpec((tokens, width), lambda i, b: (0, 0), pipeline_mode=pl.Buffered(1)),
                pl.BlockSpec((width, tokens), lambda i, b: (0, 0), pipeline_mode=pl.Buffered(1)),
                row_spec,
                row_spec,
            ],
            out_specs=[
                pl.BlockSpec((size, width), lambda i, b: (i, 0)),
                pl.BlockSpec((heads, size), lambda i, b: (0, i)),
            ],
            scratch_shapes=[
                pltpu.VMEM((heads, size, pair_width), jnp.bfloat16),
                pltpu.VMEM((width, size), jnp.float32),
                pltpu.VMEM((heads, 1, size), jnp.float32),
                pltpu.VMEM((heads, 1, size), jnp.float32),
            ],
        ),
        compiler_params=pltpu.CompilerParams(vmem_limit_bytes=40 << 20),
    )(bounds, q, k, vt, low, high)


def backward_body(
    size, heads, pair_width,
    bounds_ref, q_ref, k_ref, v_ref, kt_ref, do_ref, ctx_ref, lse_ref, low_ref, high_ref,
    dq_ref, dk_ref, dv_ref,
    qh_ref, doh_ref, delta_ref, dqt_ref, dk_acc, dv_acc,
):
    block = pl.program_id(0)
    blocks = pl.num_programs(0)
    groups = heads * HEAD_DIM // pair_width

    @pl.when(block == 0)
    def _():
        dqt_ref[...] = jnp.zeros_like(dqt_ref)

        def prepare(index, carry):
            rows = pl.ds(pl.multiple_of(index * size, size), size)
            for head in range(heads):
                qh_ref[head, rows, :] = pick_head(q_ref[rows, :], head, pair_width) * jnp.bfloat16(0.125)
                doh_ref[head, rows, :] = pick_head(do_ref[rows, :], head, pair_width)
            both = (do_ref[rows, :].astype(jnp.float32) * ctx_ref[rows, :].astype(jnp.float32)).T
            for head in range(heads):
                part = both[head * HEAD_DIM : (head + 1) * HEAD_DIM, :]
                delta_ref[head, :, rows] = jnp.sum(part, axis=0, keepdims=True)
            return carry

        lax.fori_loop(0, blocks, prepare, 0)

    dk_acc[...] = jnp.zeros_like(dk_acc)
    dv_acc[...] = jnp.zeros_like(dv_acc)
    key_start = block * size
    lower, upper = bounds_ref[4, block], bounds_ref[5, block]

    def visit(query_block, masked):
        query_start = pl.multiple_of(query_block * size, size)
        rows = pl.ds(query_start, size)
        if masked:
            allowed = allowed_tile(
                key_start, query_start, low_ref[:, rows], high_ref[:, rows], size
            )
        for head in range(heads):
            group = head * HEAD_DIM // pair_width
            lanes = slice(group * pair_width, (group + 1) * pair_width)
            query, grad = qh_ref[head, rows, :], doh_ref[head, rows, :]
            scores = dot_f32(k_ref[:, lanes], query, NT)
            weights = jnp.exp(scores - lse_ref[head : head + 1, rows])
            if masked:
                weights = jnp.where(allowed, weights, 0.0)
            dv_acc[:, lanes] += dot_f32(weights.astype(jnp.bfloat16), grad, NN)
            d_weights = dot_f32(v_ref[:, lanes], grad, NT)
            d_scores = (weights * (d_weights - delta_ref[head, :, rows])).astype(jnp.bfloat16)
            dk_acc[:, lanes] += dot_f32(d_scores, query, NN)
            feats = slice(head * HEAD_DIM, (head + 1) * HEAD_DIM)
            dqt_ref[feats, rows] += dot_f32(kt_ref[feats, :], d_scores, NN)

    def step(query_block, carry):
        full = (key_start >= bounds_ref[1, query_block]) & (
            key_start + size <= bounds_ref[2, query_block]
        )
        pl.when(full)(lambda: visit(query_block, False))
        pl.when(jnp.logical_not(full))(lambda: visit(query_block, True))
        return carry

    lax.fori_loop(lower, upper, step, 0)
    dk_ref[...] = dk_acc[...].astype(jnp.bfloat16)
    dv_ref[...] = dv_acc[...].astype(jnp.bfloat16)

    @pl.when(block == blocks - 1)
    def _():
        def finish(index, carry):
            rows = pl.ds(pl.multiple_of(index * size, size), size)
            dq_ref[rows, :] = (dqt_ref[:, rows] * 0.125).T.astype(jnp.bfloat16)
            return carry

        lax.fori_loop(0, blocks, finish, 0)


def attend_backward(q, k, v, kt, d_ctx, ctx, lse, low, high, bounds):
    tokens, width = q.shape
    size = block_size_of(tokens)
    heads = width // HEAD_DIM
    pair_width = min(128, width)
    once = pl.Buffered(1)
    whole = pl.BlockSpec((tokens, width), lambda i, b: (0, 0), pipeline_mode=once)
    block = pl.BlockSpec((size, width), lambda i, b: (i, 0))
    row = pl.BlockSpec((1, tokens), lambda i, b: (0, 0), pipeline_mode=once)
    return pl.pallas_call(
        functools.partial(backward_body, size, heads, pair_width),
        name="attend_backward",
        out_shape=[jax.ShapeDtypeStruct((tokens, width), jnp.bfloat16)] * 3,
        grid_spec=pltpu.PrefetchScalarGridSpec(
            num_scalar_prefetch=1,
            grid=(tokens // size,),
            in_specs=[
                whole, block, block,
                pl.BlockSpec((width, size), lambda i, b: (0, i)),
                whole, whole,
                pl.BlockSpec((heads, tokens), lambda i, b: (0, 0), pipeline_mode=once),
                row, row,
            ],
            out_specs=[whole, block, block],
            scratch_shapes=[
                pltpu.VMEM((heads, tokens, pair_width), jnp.bfloat16),
                pltpu.VMEM((heads, tokens, pair_width), jnp.bfloat16),
                pltpu.VMEM((heads, 1, tokens), jnp.float32),
                pltpu.VMEM((width, tokens), jnp.float32),
                pltpu.VMEM((size, width), jnp.float32),
                pltpu.VMEM((size, width), jnp.float32),
            ],
        ),
        compiler_params=pltpu.CompilerParams(vmem_limit_bytes=48 << 20),
    )(bounds, q, k, v, kt, d_ctx, ctx, lse, low, high)


def key_bounds(seg_row, valid_row, size):
    tokens = seg_row.shape[0]
    ids = jnp.arange(8, dtype=jnp.int32)
    starts = jnp.sum((seg_row[None, :] < ids[:, None]).astype(jnp.int32), axis=1)
    ends = jnp.sum((seg_row[None, :] <= ids[:, None]).astype(jnp.int32), axis=1)
    valid_count = jnp.sum(valid_row)
    member = seg_row[None, :] == ids[:, None]
    low = jnp.sum(jnp.where(member, starts[:, None], 0), axis=0)
    end = jnp.sum(jnp.where(member, ends[:, None], 0), axis=0)
    high = jnp.minimum(end, valid_count)
    first_key = jnp.arange(0, tokens, size, dtype=jnp.int32)
    own = first_key // size
    live = first_key < valid_count
    seg_blocks = seg_row.reshape(-1, size)
    last_live = jnp.minimum(first_key + size, valid_count) - 1
    last_text = jnp.sum((starts[None, :] <= last_live[:, None]).astype(jnp.int32), axis=1) - 1
    last_end = jnp.sum(jnp.where(last_text[:, None] == ids[None, :], ends[None, :], 0), axis=1)
    low_blocks, high_blocks = low.reshape(-1, size), high.reshape(-1, size)
    query_from = jnp.where(live, low_blocks[:, 0] // size, own)
    query_to = jnp.where(live, jnp.maximum((last_end + size - 1) // size, own + 1), own + 1)
    bounds = jnp.stack(
        [low_blocks[:, 0], low_blocks[:, -1], high_blocks[:, 0], high_blocks[:, -1], query_from, query_to]
    )
    return low[None, :], high[None, :], bounds


from jax.sharding import PartitionSpec as P

EPSILON = 1e-05
EVERY = ("tensor", "batch")


def inner_first(left, right):
    return dot_f32(left, right, (((0,), (0,)), ((), ())))


def inner_last(left, right):
    return dot_f32(left, right, NT)


def gelu_exact(value):
    return 0.5 * value * (1.0 + lax.erf(value * (1.0 / math.sqrt(2.0))))


def norm_stats(value):
    mean_value = jnp.mean(value, axis=1, keepdims=True)
    spread = jnp.mean(value * value, axis=1, keepdims=True) - mean_value * mean_value
    return mean_value, lax.rsqrt(spread + EPSILON)


def norm_backward(d_scaled, normed, scale):
    return scale * (
        d_scaled
        - jnp.mean(d_scaled, axis=1, keepdims=True)
        - normed * jnp.mean(d_scaled * normed, axis=1, keepdims=True)
    )


def batch_piece(weight):
    rows = weight.shape[0] // lax.axis_size("batch")
    return lax.dynamic_slice_in_dim(weight, lax.axis_index("batch") * rows, rows, 0)


def gather_weight(weight):
    return lax.all_gather(batch_piece(weight), EVERY, axis=0, tiled=True)


def heads_to_tokens(value):
    return lax.all_to_all(value, "tensor", split_axis=0, concat_axis=1, tiled=True)


def tokens_to_heads(value):
    return lax.all_to_all(value, "tensor", split_axis=1, concat_axis=0, tiled=True)


def reduce_weight(grad):
    part = lax.psum_scatter(grad.astype(jnp.bfloat16), "batch", scatter_dimension=0, tiled=True)
    return part


def local(
    inputs,
    segments,
    valid,
    w_query,
    b_query,
    w_key,
    w_value,
    b_value,
    w_out,
    b_out,
    gain_one,
    shift_one,
    w_up,
    b_up,
    w_down,
    b_down,
    gain_two,
    shift_two,
    lex_weight,
    lex_bias,
    cotangent,
):
    row_count, seq_len, full_width = inputs.shape
    token_count = row_count * seq_len
    shards = lax.axis_size("tensor")
    members = lax.axis_size("batch")
    me = lax.axis_index("tensor")
    slice_width = full_width // shards
    own_count = token_count // shards
    flat = inputs.reshape(token_count, full_width)
    size = block_size_of(seq_len)

    out_full = gather_weight(w_out)
    up_full = gather_weight(w_up.T)
    down_full = gather_weight(w_down)
    small = jnp.concatenate(
        [b_out, gain_one, shift_one, b_down, gain_two, shift_two, lex_weight, b_up]
    )
    small_all = lax.all_gather(small, "tensor", axis=0).astype(jnp.float32)
    vectors = [
        small_all[:, i * slice_width : (i + 1) * slice_width].reshape(1, full_width)
        for i in range(7)
    ]
    b_out_v, gain_one_v, shift_one_v, b_down_v, gain_two_v, shift_two_v, lex_v = vectors
    b_up_v = small_all[:, 7 * slice_width :].reshape(1, -1)

    queries = (jnp.dot(flat, w_query, preferred_element_type=jnp.float32) + b_query).astype(
        jnp.bfloat16
    )
    key_rows = jnp.dot(flat, w_key, preferred_element_type=jnp.float32).astype(jnp.bfloat16)
    value_rows = (jnp.dot(flat, w_value, preferred_element_type=jnp.float32) + b_value).astype(
        jnp.bfloat16
    )
    d_final = heads_to_tokens(cotangent.reshape(token_count, slice_width)).astype(jnp.float32)
    rows = []
    for row in range(row_count):
        span = slice(row * seq_len, (row + 1) * seq_len)
        low, high, bounds = key_bounds(segments[row], valid[row], size)
        row_q, row_k, row_v = queries[span], key_rows[span], value_rows[span]
        row_ctx, row_lse = attend_forward(row_q, row_k, row_v.T, low, high, bounds)
        rows.append((row_q, row_k, row_v, row_ctx, row_lse, low, high, bounds))
    context = jnp.concatenate([item[3] for item in rows], axis=0)

    token_ctx = heads_to_tokens(context)
    own_input = lax.dynamic_slice_in_dim(flat, me * own_count, own_count, 0).astype(jnp.float32)
    first_res = own_input + jnp.dot(token_ctx, out_full, preferred_element_type=jnp.float32) + b_out_v
    mean_one, scale_one = norm_stats(first_res)
    normed_one = (first_res - mean_one) * scale_one
    first_out = normed_one * gain_one_v + shift_one_v
    first_low = first_out.astype(jnp.bfloat16)
    pre_up = inner_last(first_low, up_full) + b_up_v
    hidden = gelu_exact(pre_up).astype(jnp.bfloat16)
    second_res = first_out + jnp.dot(hidden, down_full, preferred_element_type=jnp.float32) + b_down_v
    mean_two, scale_two = norm_stats(second_res)
    normed_two = (second_res - mean_two) * scale_two
    final_out = normed_two * gain_two_v + shift_two_v
    output = tokens_to_heads(final_out.astype(jnp.bfloat16))
    lex_pre = jnp.sum(final_out * lex_v, axis=1) + lex_bias[0].astype(jnp.float32)
    valid_float = lax.dynamic_slice_in_dim(
        valid.reshape(token_count), me * own_count, own_count, 0
    ).astype(jnp.float32)
    lex_totals = jnp.stack(
        [
            jnp.sum(valid_float),
            jnp.sum(jnp.maximum(lex_pre, 0.0) * valid_float),
            jnp.sum(jnp.where(lex_pre > 0.0, valid_float, 0.0)),
        ]
    )

    grad_gain_two = jnp.sum(d_final * normed_two, axis=0)
    grad_shift_two = jnp.sum(d_final, axis=0)
    d_second = norm_backward(d_final * gain_two_v, normed_two, scale_two)
    grad_b_down = jnp.sum(d_second, axis=0)
    d_ffn_low = d_second.astype(jnp.bfloat16)
    d_hidden = inner_last(d_ffn_low, down_full)
    _, gelu_back = jax.vjp(gelu_exact, pre_up)
    d_pre_up = gelu_back(d_hidden)[0].astype(jnp.bfloat16)
    grad_b_up = jnp.sum(d_pre_up, axis=0, dtype=jnp.float32)
    d_first = d_second + jnp.dot(d_pre_up, up_full, preferred_element_type=jnp.float32)
    grad_gain_one = jnp.sum(d_first * normed_one, axis=0)
    grad_shift_one = jnp.sum(d_first, axis=0)
    d_first_res = norm_backward(d_first * gain_one_v, normed_one, scale_one)
    grad_b_out = jnp.sum(d_first_res, axis=0)
    d_attn_low = d_first_res.astype(jnp.bfloat16)
    d_context = tokens_to_heads(inner_last(d_attn_low, out_full).astype(jnp.bfloat16))

    weight_grads = []
    for left, right in ((hidden, d_ffn_low), (d_pre_up, first_low), (token_ctx, d_attn_low)):
        grad = inner_first(left, right)
        grad = grad.reshape(shards, members, -1, full_width).transpose(1, 0, 2, 3)
        part = lax.psum_scatter(
            grad.astype(jnp.bfloat16), "batch", scatter_dimension=0, tiled=True
        )[0]
        part = lax.psum_scatter(part, "tensor", scatter_dimension=0, tiled=True)[0]
        weight_grads.append(
            lax.all_gather(part, "batch", axis=0, tiled=True).astype(jnp.float32)
        )
    grad_w_down, grad_w_up_t, grad_w_out = weight_grads
    token_sums = jnp.concatenate(
        [
            item.reshape(shards, -1)
            for item in (
                grad_b_out,
                grad_gain_one,
                grad_shift_one,
                grad_b_down,
                grad_gain_two,
                grad_shift_two,
                grad_b_up,
                jnp.broadcast_to(lex_totals, (shards, 3)),
            )
        ],
        axis=1,
    )
    own_sums = lax.dynamic_index_in_dim(lax.psum(token_sums, EVERY), me, 0, False)
    sums = [own_sums[i * slice_width : (i + 1) * slice_width] for i in range(6)]
    sum_b_up = own_sums[6 * slice_width : -3]
    totals_all = own_sums[-3:]
    lex_stats = jnp.stack([totals_all[1] / totals_all[0], totals_all[2] / totals_all[0]])

    grads = []
    for row in range(row_count):
        row_q, row_k, row_v, row_ctx, row_lse, low, high, bounds = rows[row]
        grads.append(
            attend_backward(
                row_q, row_k, row_v, row_k.T,
                d_context[row * seq_len : (row + 1) * seq_len],
                row_ctx, row_lse, low, high, bounds,
            )
        )
    d_queries, d_keys, d_values = (
        jnp.concatenate([item[i] for item in grads], axis=0) for i in range(3)
    )
    d_input_term = (
        inner_last(d_queries, w_query) + inner_last(d_keys, w_key) + inner_last(d_values, w_value)
    )
    own_term = lax.dynamic_slice_in_dim(d_input_term, me * own_count, own_count, 0) + d_first_res
    d_input_term = lax.dynamic_update_slice_in_dim(
        d_input_term.astype(jnp.bfloat16), own_term.astype(jnp.bfloat16), me * own_count, 0
    )
    grad_inputs = lax.psum_scatter(d_input_term, "tensor", scatter_dimension=1, tiled=True)
    head_sums = [
        inner_first(flat, d_queries),
        inner_first(flat, d_keys),
        inner_first(flat, d_values),
        jnp.sum(d_queries, axis=0, dtype=jnp.float32),
        jnp.sum(d_values, axis=0, dtype=jnp.float32),
    ]
    head_sums = [
        lax.psum(item.astype(jnp.bfloat16), "batch").astype(jnp.float32) for item in head_sums
    ]
    out_shape = (row_count, seq_len, slice_width)
    return (
        output.reshape(out_shape),
        grad_inputs.reshape(out_shape),
        head_sums[0],
        head_sums[3],
        head_sums[1],
        head_sums[2],
        head_sums[4],
        grad_w_out,
        sums[0],
        sums[1],
        sums[2],
        grad_w_up_t.T,
        sum_b_up,
        grad_w_down,
        sums[3],
        sums[4],
        sums[5],
        lex_stats,
    )


def solution(mesh):
    in_specs = (
        P("batch", None, None),
        P("batch", None),
        P("batch", None),
        P(None, "tensor"),
        P("tensor"),
        P(None, "tensor"),
        P(None, "tensor"),
        P("tensor"),
        P("tensor", None),
        P("tensor"),
        P("tensor"),
        P("tensor"),
        P(None, "tensor"),
        P("tensor"),
        P("tensor", None),
        P("tensor"),
        P("tensor"),
        P("tensor"),
        P("tensor"),
        P(),
        P("batch", None, "tensor"),
    )
    out_specs = (
        P("batch", None, "tensor"),
        P("batch", None, "tensor"),
        P(None, "tensor"),
        P("tensor"),
        P(None, "tensor"),
        P(None, "tensor"),
        P("tensor"),
        P("tensor", None),
        P("tensor"),
        P("tensor"),
        P("tensor"),
        P(None, "tensor"),
        P("tensor"),
        P("tensor", None),
        P("tensor"),
        P("tensor"),
        P("tensor"),
        P(),
    )
    return jax.shard_map(local, mesh=mesh, in_specs=in_specs, out_specs=out_specs, check_vma=False)
```

```python
import math, functools
import jax
import jax.numpy as jnp
from jax import lax
from jax.experimental import pallas as pl
from jax.experimental.pallas import tpu as pltpu

HEAD_DIM = 64
MASKED = -1e30
NT = (((1,), (1,)), ((), ()))
NN = (((1,), (0,)), ((), ()))


def dot_f32(left, right, dims):
    return lax.dot_general(left, right, dims, preferred_element_type=jnp.float32)


def head_lanes(shape, slot):
    lane = lax.broadcasted_iota(jnp.int32, shape, 1)
    return (lane >= slot * HEAD_DIM) & (lane < (slot + 1) * HEAD_DIM)


def pick_head(block, head, pair_width):
    group, slot = divmod(head * HEAD_DIM, pair_width)
    pair = block[:, group * pair_width : (group + 1) * pair_width]
    if pair_width == HEAD_DIM:
        return pair
    return jnp.where(head_lanes(pair.shape, slot // HEAD_DIM), pair, jnp.zeros_like(pair))


def allowed_tile(key_start, query_start, low_row, high_row, size):
    key_pos = key_start + lax.broadcasted_iota(jnp.int32, (size, 1), 0)
    query_pos = query_start + lax.broadcasted_iota(jnp.int32, (1, size), 1)
    return ((key_pos >= low_row) & (key_pos < high_row)) | (key_pos == query_pos)


def forward_body(
    first_block, size, heads, pair_width,
    bounds_ref, q_ref, k_ref, vt_ref, low_ref, high_ref,
    ctx_ref, lse_ref,
    qh_ref, acc_ref, max_ref, sum_ref,
):
    block = first_block + pl.program_id(0)
    for head in range(heads):
        qh_ref[head] = pick_head(q_ref[...], head, pair_width) * jnp.bfloat16(0.125)
    acc_ref[...] = jnp.zeros_like(acc_ref)
    max_ref[...] = jnp.full_like(max_ref, MASKED)
    sum_ref[...] = jnp.zeros_like(sum_ref)
    low_first, low_last = bounds_ref[0, block], bounds_ref[1, block]
    high_first, high_last = bounds_ref[2, block], bounds_ref[3, block]
    lower = low_first // size
    count = jnp.maximum((high_last + size - 1) // size - lower, 0)
    extra = jnp.where(block < lower + count, 0, 1)

    def visit(key_block, masked):
        key_start = pl.multiple_of(key_block * size, size)
        keys = pl.ds(key_start, size)
        if masked:
            allowed = allowed_tile(
                key_start, block * size, low_ref[...], high_ref[...], size
            )
        raw = []
        for head in range(heads):
            base = head * HEAD_DIM // pair_width * pair_width
            raw.append(dot_f32(k_ref[keys, base : base + pair_width], qh_ref[head], NT))
        old_max = [max_ref[head] for head in range(heads)]
        old_sum = [sum_ref[head] for head in range(heads)]
        new_max, new_sum, scales, low_expo = [], [], [], []
        for head in range(heads):
            scores = jnp.where(allowed, raw[head], MASKED) if masked else raw[head]
            top = jnp.maximum(old_max[head], jnp.max(scores, axis=0, keepdims=True))
            expo = jnp.exp(scores - top)
            scale = jnp.exp(old_max[head] - top)
            new_max.append(top)
            scales.append(scale)
            new_sum.append(old_sum[head] * scale + jnp.sum(expo, axis=0, keepdims=True))
            low_expo.append(expo.astype(jnp.bfloat16))
        terms = [
            dot_f32(vt_ref[head * HEAD_DIM : (head + 1) * HEAD_DIM, keys], low_expo[head], NN)
            for head in range(heads)
        ]
        for head in range(heads):
            rows = slice(head * HEAD_DIM, (head + 1) * HEAD_DIM)
            acc_ref[rows, :] = acc_ref[rows, :] * scales[head] + terms[head]
            max_ref[head] = new_max[head]
            sum_ref[head] = new_sum[head]

    def step(index, carry):
        key_block = jnp.where(index < count, lower + index, block)
        key_start = key_block * size
        full = (key_start >= low_last) & (key_start + size <= high_first)
        pl.when(full)(lambda: visit(key_block, False))
        pl.when(jnp.logical_not(full))(lambda: visit(key_block, True))
        return carry

    lax.fori_loop(0, count + extra, step, 0)
    for head in range(heads):
        rows = slice(head * HEAD_DIM, (head + 1) * HEAD_DIM)
        acc_ref[rows, :] = acc_ref[rows, :] / sum_ref[head]
        lse_ref[head : head + 1, :] = max_ref[head] + jnp.log(sum_ref[head])
    ctx_ref[...] = acc_ref[...].T.astype(jnp.bfloat16)


def block_size_of(tokens):
    return min(256, tokens)


def attend_forward(q, k, vt, low, high, bounds, first=0, last=None):
    tokens, width = q.shape
    size = block_size_of(tokens)
    heads = width // HEAD_DIM
    pair_width = min(128, width)
    last = tokens // size if last is None else last
    grid = last - first
    row_spec = pl.BlockSpec((1, size), lambda i, b: (0, i + first))
    return pl.pallas_call(
        functools.partial(forward_body, first, size, heads, pair_width),
        name="attend_forward",
        out_shape=(
            jax.ShapeDtypeStruct((grid * size, width), jnp.bfloat16),
            jax.ShapeDtypeStruct((heads, grid * size), jnp.float32),
        ),
        grid_spec=pltpu.PrefetchScalarGridSpec(
            num_scalar_prefetch=1,
            grid=(grid,),
            in_specs=[
                pl.BlockSpec((size, width), lambda i, b: (i + first, 0)),
                pl.BlockSpec((tokens, width), lambda i, b: (0, 0), pipeline_mode=pl.Buffered(1)),
                pl.BlockSpec((width, tokens), lambda i, b: (0, 0), pipeline_mode=pl.Buffered(1)),
                row_spec,
                row_spec,
            ],
            out_specs=[
                pl.BlockSpec((size, width), lambda i, b: (i, 0)),
                pl.BlockSpec((heads, size), lambda i, b: (0, i)),
            ],
            scratch_shapes=[
                pltpu.VMEM((heads, size, pair_width), jnp.bfloat16),
                pltpu.VMEM((width, size), jnp.float32),
                pltpu.VMEM((heads, 1, size), jnp.float32),
                pltpu.VMEM((heads, 1, size), jnp.float32),
            ],
        ),
        compiler_params=pltpu.CompilerParams(vmem_limit_bytes=40 << 20),
        cost_estimate=pl.CostEstimate(
            flops=8 * grid * size * tokens * width, transcendentals=0, bytes_accessed=6 * tokens * width
        ),
    )(bounds, q, k, vt, low, high)


def backward_body(
    first_block, is_first, is_last, size, heads, pair_width, all_blocks,
    bounds_ref, q_ref, k_ref, v_ref, kt_ref, do_ref, ctx_ref, lse_ref, low_ref, high_ref,
    *refs,
):
    carried_ref = None if is_first else refs[0]
    dq_ref, dk_ref, dv_ref, qh_ref, doh_ref, delta_ref = refs[0 if is_first else 1 :][:6]
    dk_acc, dv_acc = refs[-2:]
    dqt_ref = refs[-3] if is_last else dq_ref
    step_index = pl.program_id(0)
    block = first_block + step_index

    @pl.when(step_index == 0)
    def _():
        dqt_ref[...] = jnp.zeros_like(dqt_ref) if is_first else carried_ref[...]

        def prepare(index, carry):
            rows = pl.ds(pl.multiple_of(index * size, size), size)
            for head in range(heads):
                qh_ref[head, rows, :] = pick_head(q_ref[rows, :], head, pair_width) * jnp.bfloat16(0.125)
                doh_ref[head, rows, :] = pick_head(do_ref[rows, :], head, pair_width)
            both = (do_ref[rows, :].astype(jnp.float32) * ctx_ref[rows, :].astype(jnp.float32)).T
            for head in range(heads):
                part = both[head * HEAD_DIM : (head + 1) * HEAD_DIM, :]
                delta_ref[head, :, rows] = jnp.sum(part, axis=0, keepdims=True)
            return carry

        lax.fori_loop(0, all_blocks, prepare, 0)

    dk_acc[...] = jnp.zeros_like(dk_acc)
    dv_acc[...] = jnp.zeros_like(dv_acc)
    key_start = block * size
    lower, upper = bounds_ref[4, block], bounds_ref[5, block]

    def visit(query_block, masked):
        query_start = pl.multiple_of(query_block * size, size)
        rows = pl.ds(query_start, size)
        if masked:
            allowed = allowed_tile(
                key_start, query_start, low_ref[:, rows], high_ref[:, rows], size
            )
        for head in range(heads):
            group = head * HEAD_DIM // pair_width
            lanes = slice(group * pair_width, (group + 1) * pair_width)
            query, grad = qh_ref[head, rows, :], doh_ref[head, rows, :]
            scores = dot_f32(k_ref[:, lanes], query, NT)
            weights = jnp.exp(scores - lse_ref[head : head + 1, rows])
            if masked:
                weights = jnp.where(allowed, weights, 0.0)
            dv_acc[:, lanes] += dot_f32(weights.astype(jnp.bfloat16), grad, NN)
            d_weights = dot_f32(v_ref[:, lanes], grad, NT)
            d_scores = (weights * (d_weights - delta_ref[head, :, rows])).astype(jnp.bfloat16)
            dk_acc[:, lanes] += dot_f32(d_scores, query, NN)
            feats = slice(head * HEAD_DIM, (head + 1) * HEAD_DIM)
            dqt_ref[feats, rows] += dot_f32(kt_ref[feats, :], d_scores, NN)

    def step(query_block, carry):
        full = (key_start >= bounds_ref[1, query_block]) & (
            key_start + size <= bounds_ref[2, query_block]
        )
        pl.when(full)(lambda: visit(query_block, False))
        pl.when(jnp.logical_not(full))(lambda: visit(query_block, True))
        return carry

    lax.fori_loop(lower, upper, step, 0)
    dk_ref[...] = dk_acc[...].astype(jnp.bfloat16)
    dv_ref[...] = dv_acc[...].astype(jnp.bfloat16)

    if is_last:

        @pl.when(step_index == pl.num_programs(0) - 1)
        def _():
            def finish(index, carry):
                rows = pl.ds(pl.multiple_of(index * size, size), size)
                dq_ref[rows, :] = (dqt_ref[:, rows] * 0.125).T.astype(jnp.bfloat16)
                return carry

            lax.fori_loop(0, all_blocks, finish, 0)


def attend_backward(q, k, v, kt, d_ctx, ctx, lse, low, high, bounds, part, parts, carried):
    tokens, width = q.shape
    size = block_size_of(tokens)
    heads = width // HEAD_DIM
    pair_width = min(128, width)
    all_blocks = tokens // size
    grid = all_blocks // parts
    first = part * grid
    is_first, is_last = part == 0, part == parts - 1
    once = pl.Buffered(1)
    whole = pl.BlockSpec((tokens, width), lambda i, b: (0, 0), pipeline_mode=once)
    turned = pl.BlockSpec((width, tokens), lambda i, b: (0, 0), pipeline_mode=once)
    block = pl.BlockSpec((size, width), lambda i, b: (i + first, 0))
    block_out = pl.BlockSpec((size, width), lambda i, b: (i, 0))
    row = pl.BlockSpec((1, tokens), lambda i, b: (0, 0), pipeline_mode=once)
    part_shape = jax.ShapeDtypeStruct((grid * size, width), jnp.bfloat16)
    query_grad = (
        jax.ShapeDtypeStruct((tokens, width), jnp.bfloat16)
        if is_last
        else jax.ShapeDtypeStruct((width, tokens), jnp.float32)
    )
    scratch = [
        pltpu.VMEM((heads, tokens, pair_width), jnp.bfloat16),
        pltpu.VMEM((heads, tokens, pair_width), jnp.bfloat16),
        pltpu.VMEM((heads, 1, tokens), jnp.float32),
    ]
    if is_last:
        scratch.append(pltpu.VMEM((width, tokens), jnp.float32))
    scratch += [pltpu.VMEM((size, width), jnp.float32)] * 2
    operands = [bounds, q, k, v, kt, d_ctx, ctx, lse, low, high]
    in_specs = [
        whole, block, block,
        pl.BlockSpec((width, size), lambda i, b: (0, i + first)),
        whole, whole,
        pl.BlockSpec((heads, tokens), lambda i, b: (0, 0), pipeline_mode=once),
        row, row,
    ]
    if not is_first:
        operands.append(carried)
        in_specs.append(turned)
    return pl.pallas_call(
        functools.partial(
            backward_body, first, is_first, is_last, size, heads, pair_width, all_blocks
        ),
        name="attend_backward",
        out_shape=[query_grad, part_shape, part_shape],
        grid_spec=pltpu.PrefetchScalarGridSpec(
            num_scalar_prefetch=1,
            grid=(grid,),
            in_specs=in_specs,
            out_specs=[whole if is_last else turned, block_out, block_out],
            scratch_shapes=scratch,
        ),
        compiler_params=pltpu.CompilerParams(vmem_limit_bytes=48 << 20),
        cost_estimate=pl.CostEstimate(
            flops=20 * grid * size * tokens * width, transcendentals=0, bytes_accessed=20 * tokens * width
        ),
    )(*operands)


def key_bounds(seg_row, valid_row, size):
    tokens = seg_row.shape[0]
    ids = jnp.arange(8, dtype=jnp.int32)
    starts = jnp.sum((seg_row[None, :] < ids[:, None]).astype(jnp.int32), axis=1)
    ends = jnp.sum((seg_row[None, :] <= ids[:, None]).astype(jnp.int32), axis=1)
    valid_count = jnp.sum(valid_row)
    member = seg_row[None, :] == ids[:, None]
    low = jnp.sum(jnp.where(member, starts[:, None], 0), axis=0)
    end = jnp.sum(jnp.where(member, ends[:, None], 0), axis=0)
    high = jnp.minimum(end, valid_count)
    first_key = jnp.arange(0, tokens, size, dtype=jnp.int32)
    own = first_key // size
    live = first_key < valid_count
    seg_blocks = seg_row.reshape(-1, size)
    last_live = jnp.minimum(first_key + size, valid_count) - 1
    last_text = jnp.sum((starts[None, :] <= last_live[:, None]).astype(jnp.int32), axis=1) - 1
    last_end = jnp.sum(jnp.where(last_text[:, None] == ids[None, :], ends[None, :], 0), axis=1)
    low_blocks, high_blocks = low.reshape(-1, size), high.reshape(-1, size)
    query_from = jnp.where(live, low_blocks[:, 0] // size, own)
    query_to = jnp.where(live, jnp.maximum((last_end + size - 1) // size, own + 1), own + 1)
    bounds = jnp.stack(
        [low_blocks[:, 0], low_blocks[:, -1], high_blocks[:, 0], high_blocks[:, -1], query_from, query_to]
    )
    return low[None, :], high[None, :], bounds


from jax.sharding import PartitionSpec as P

EPSILON = 1e-05
PARTS = 4


def inner_first(left, right):
    return dot_f32(left, right, (((0,), (0,)), ((), ())))


def inner_last(left, right):
    return dot_f32(left, right, NT)


def gelu_exact(value):
    return 0.5 * value * (1.0 + lax.erf(value * (1.0 / math.sqrt(2.0))))


def norm_stats(value):
    mean_value = jnp.mean(value, axis=1, keepdims=True)
    spread = jnp.mean(value * value, axis=1, keepdims=True) - mean_value * mean_value
    return mean_value, lax.rsqrt(spread + EPSILON)


def norm_backward(d_scaled, normed, scale):
    return scale * (
        d_scaled
        - jnp.mean(d_scaled, axis=1, keepdims=True)
        - normed * jnp.mean(d_scaled * normed, axis=1, keepdims=True)
    )


def flip(value, bit):
    members = lax.axis_size("batch")
    return lax.ppermute(value, "batch", [(i, i ^ (1 << bit)) for i in range(members)])


def shift(value, step):
    shards = lax.axis_size("tensor")
    return lax.ppermute(value, "tensor", [(i, (i + step) % shards) for i in range(shards)])


def heads_to_tokens(value):
    return lax.all_to_all(value, "tensor", split_axis=0, concat_axis=1, tiled=True)


def tokens_to_heads(value):
    return lax.all_to_all(value, "tensor", split_axis=1, concat_axis=0, tiled=True)


def bit_orders():
    bits = list(range(1, lax.axis_size("batch").bit_length() - 1))
    return bits, bits[::-1]


def tie(value, others):
    return lax.optimization_barrier((value, others))


def gather_step(chunks, bit):
    moved = {j | (1 << bit): flip(chunk, bit) for j, chunk in chunks.items()}
    return {**chunks, **moved}


def reduce_step(chunks, bit):
    moved = {j: flip(chunk, bit) for j, chunk in chunks.items() if j >> bit & 1}
    return {
        j: add_low(chunk, moved[j | (1 << bit)]) for j, chunk in chunks.items() if not j >> bit & 1
    }


def add_low(left, right):
    return (left.astype(jnp.float32) + right.astype(jnp.float32)).astype(left.dtype)


def sum_members(value, order):
    for bit in [0] + order:
        value = add_low(value, flip(value, bit))
    return value


def gather_shards(piece):
    return [piece] + [shift(piece, s) for s in range(1, lax.axis_size("tensor"))]


def reduce_shards(blocks):
    total = blocks[0].astype(jnp.float32)
    for s in range(1, len(blocks)):
        total = total + shift(blocks[s], -s).astype(jnp.float32)
    return total


def in_order(blocks, buffer_shape, axis, index_of):
    result = jnp.zeros(buffer_shape, blocks[0].dtype)
    for s, block in enumerate(blocks):
        result = lax.dynamic_update_slice_in_dim(
            result, jnp.expand_dims(block, axis), index_of(s), axis
        )
    return result


def local(
    inputs,
    segments,
    valid,
    w_query,
    b_query,
    w_key,
    w_value,
    b_value,
    w_out,
    b_out,
    gain_one,
    shift_one,
    w_up,
    b_up,
    w_down,
    b_down,
    gain_two,
    shift_two,
    lex_weight,
    lex_bias,
    cotangent,
):
    row_count, seq_len, full_width = inputs.shape
    token_count = row_count * seq_len
    shards = lax.axis_size("tensor")
    members = lax.axis_size("batch")
    me = lax.axis_index("tensor")
    local_width = w_query.shape[1]
    slice_width = full_width // shards
    own_count = token_count // shards
    flat = inputs.reshape(token_count, full_width)
    size = block_size_of(seq_len)

    parts = PARTS if seq_len % (PARTS * shards * 8) == 0 else 1
    part_len = seq_len // parts
    own_len = part_len // shards
    first_order, second_order = bit_orders()
    member = lax.axis_index("batch")
    piece_len = w_down.shape[0] // members

    def own_tokens(value):
        split = value.reshape((row_count * parts, shards, own_len) + value.shape[1:])
        picked = lax.dynamic_index_in_dim(split, me, 1, False)
        return picked.reshape((own_count,) + value.shape[1:])

    small = jnp.concatenate(
        [b_out, gain_one, shift_one, b_down, gain_two, shift_two, lex_weight, b_up]
    )
    small_all = in_order(
        gather_shards(small), (shards,) + small.shape, 0, lambda s: (me - s) % shards
    ).astype(jnp.float32)
    vectors = [
        small_all[:, i * slice_width : (i + 1) * slice_width].reshape(1, full_width)
        for i in range(7)
    ]
    b_out_v, gain_one_v, shift_one_v, b_down_v, gain_two_v, shift_two_v, lex_v = vectors
    shard_order = (me - jnp.arange(shards)) % shards
    member_order = member ^ jnp.arange(members)
    b_up_all = small_all[:, 7 * slice_width :].reshape(shards, members, piece_len)
    b_up_all = jnp.take(jnp.take(b_up_all, shard_order, axis=0), member_order, axis=1)

    up_piece = lax.dynamic_slice_in_dim(w_up, member * piece_len, piece_len, 1).T
    down_piece = lax.dynamic_slice_in_dim(w_down, member * piece_len, piece_len, 0)
    both = gather_shards(jnp.stack([up_piece, down_piece]))
    out_blocks = gather_shards(w_out)
    up_chunks = {0: jnp.concatenate([item[0] for item in both], axis=0)}
    down_chunks = {0: jnp.concatenate([item[1] for item in both], axis=0)}
    gather_bits = list(zip(first_order, second_order)) + [(0, 0)]

    queries = (jnp.dot(flat, w_query, preferred_element_type=jnp.float32) + b_query).astype(
        jnp.bfloat16
    )
    key_rows = jnp.dot(flat, w_key, preferred_element_type=jnp.float32).astype(jnp.bfloat16)
    value_rows = (jnp.dot(flat, w_value, preferred_element_type=jnp.float32) + b_value).astype(
        jnp.bfloat16
    )
    split_cot = cotangent.reshape(row_count * parts, shards, own_len, slice_width)
    split_cot = split_cot.transpose(1, 0, 2, 3).reshape(token_count, slice_width)
    split_cot, (up_chunks, down_chunks, out_blocks) = tie(
        split_cot, (up_chunks, down_chunks, out_blocks)
    )
    d_final = heads_to_tokens(split_cot)
    rows = []
    arrived = []
    for row in range(row_count):
        span = slice(row * seq_len, (row + 1) * seq_len)
        low, high, bounds = key_bounds(segments[row], valid[row], size)
        row_q, row_k, row_v = queries[span], key_rows[span], value_rows[span]
        row_vt = row_v.T
        pieces = []
        for part in range(parts):
            if row == 0 and part > 0:
                row_q, (up_chunks, down_chunks) = tie(row_q, (up_chunks, down_chunks))
                if part == parts - 1:
                    row_q, d_final = tie(row_q, d_final)
                if part > 1:
                    row_q, arrived[part - 2] = tie(row_q, arrived[part - 2])
                if gather_bits:
                    up_bit, down_bit = gather_bits.pop(0)
                    up_chunks = gather_step(up_chunks, up_bit)
                    down_chunks = gather_step(down_chunks, down_bit)
            part_blocks = part_len // size
            piece = attend_forward(
                row_q, row_k, row_vt, low, high, bounds,
                part * part_blocks, (part + 1) * part_blocks,
            )
            pieces.append(piece)
            sent = piece[0].reshape(shards, own_len, local_width)
            slots = [lax.dynamic_index_in_dim(sent, me, 0, False)]
            for s in range(1, shards):
                slots.append(
                    shift(lax.dynamic_index_in_dim(sent, (me + s) % shards, 0, False), s)
                )
            arrived.append(slots)
        row_ctx = jnp.concatenate([item[0] for item in pieces], axis=0)
        row_lse = jnp.concatenate([item[1] for item in pieces], axis=1)
        rows.append((row_q, row_k, row_v, row_ctx, row_lse, low, high, bounds))
    for up_bit, down_bit in gather_bits:
        up_chunks = gather_step(up_chunks, up_bit)
        down_chunks = gather_step(down_chunks, down_bit)
    up_full = jnp.concatenate([up_chunks[j] for j in range(members)], axis=0)
    down_full = jnp.concatenate([down_chunks[j] for j in range(members)], axis=0)
    d_final = d_final.astype(jnp.float32)
    token_ctx = [jnp.concatenate([item[s] for item in arrived], axis=0) for s in range(shards)]

    first_res = own_tokens(flat).astype(jnp.float32) + b_out_v
    for left, right in zip(token_ctx, out_blocks):
        first_res = first_res + dot_f32(left, right, NN)
    mean_one, scale_one = norm_stats(first_res)
    normed_one = (first_res - mean_one) * scale_one
    first_out = normed_one * gain_one_v + shift_one_v
    first_low = first_out.astype(jnp.bfloat16)
    b_up_v = b_up_all.transpose(1, 0, 2).reshape(1, -1)
    pre_up = inner_last(first_low, up_full) + b_up_v
    hidden = gelu_exact(pre_up).astype(jnp.bfloat16)
    second_res = first_out + jnp.dot(hidden, down_full, preferred_element_type=jnp.float32) + b_down_v
    mean_two, scale_two = norm_stats(second_res)
    normed_two = (second_res - mean_two) * scale_two
    final_out = normed_two * gain_two_v + shift_two_v
    output = final_out.astype(jnp.bfloat16)
    lex_pre = jnp.sum(final_out * lex_v, axis=1) + lex_bias[0].astype(jnp.float32)
    valid_float = own_tokens(valid.reshape(token_count)).astype(jnp.float32)
    lex_totals = jnp.stack(
        [
            jnp.sum(valid_float),
            jnp.sum(jnp.maximum(lex_pre, 0.0) * valid_float),
            jnp.sum(jnp.where(lex_pre > 0.0, valid_float, 0.0)),
        ]
    )

    grad_gain_two = jnp.sum(d_final * normed_two, axis=0)
    grad_shift_two = jnp.sum(d_final, axis=0)
    d_second = norm_backward(d_final * gain_two_v, normed_two, scale_two)
    grad_b_down = jnp.sum(d_second, axis=0)
    d_ffn_low = d_second.astype(jnp.bfloat16)
    d_hidden = inner_last(d_ffn_low, down_full)
    _, gelu_back = jax.vjp(gelu_exact, pre_up)
    d_pre_up = gelu_back(d_hidden)[0].astype(jnp.bfloat16)
    d_first = d_second + jnp.dot(d_pre_up, up_full, preferred_element_type=jnp.float32)
    grad_b_up = jnp.sum(d_pre_up, axis=0, dtype=jnp.float32)
    grad_b_up = grad_b_up.reshape(members, shards, piece_len).transpose(1, 0, 2)
    grad_b_up = jnp.take(jnp.take(grad_b_up, shard_order, axis=0), member_order, axis=1)
    grad_gain_one = jnp.sum(d_first * normed_one, axis=0)
    grad_shift_one = jnp.sum(d_first, axis=0)
    d_first_res = norm_backward(d_first * gain_one_v, normed_one, scale_one)
    grad_b_out = jnp.sum(d_first_res, axis=0)
    d_attn_low = d_first_res.astype(jnp.bfloat16)
    terms = [inner_last(d_attn_low, block).astype(jnp.bfloat16) for block in out_blocks]
    (d_ffn_late, first_late, d_attn_late), terms = tie((d_ffn_low, first_low, d_attn_low), terms)
    back = [term if s == 0 else shift(term, -s) for s, term in enumerate(terms)]
    d_context = in_order(
        [item.reshape(row_count * parts, own_len, local_width) for item in back],
        (row_count * parts, shards, own_len, local_width),
        1,
        lambda s: (me + s) % shards,
    ).reshape(token_count, local_width)

    def weight_grad(left, right):
        return inner_first(left, right).astype(jnp.bfloat16)

    chunk_len = shards * piece_len
    spans = [slice(j * chunk_len, (j + 1) * chunk_len) for j in range(members)]
    down_grads = {j: weight_grad(hidden[:, spans[j]], d_ffn_late) for j in range(members)}
    up_grads = {j: weight_grad(d_pre_up[:, spans[j]], first_late) for j in range(members)}
    out_grads = [weight_grad(item, d_attn_late) for item in token_ctx]
    d_context, (down_grads, up_grads, out_grads) = tie(
        d_context, (down_grads, up_grads, out_grads)
    )
    output, d_context = tie(output, d_context)
    output = tokens_to_heads(output)
    token_sums = jnp.concatenate(
        [
            item.reshape(shards, -1)
            for item in (
                grad_b_out,
                grad_gain_one,
                grad_shift_one,
                grad_b_down,
                grad_gain_two,
                grad_shift_two,
                grad_b_up,
                jnp.broadcast_to(lex_totals, (shards, 3)),
            )
        ],
        axis=1,
    )
    own_sums = reduce_shards(
        [lax.dynamic_index_in_dim(token_sums, (me - s) % shards, 0, False) for s in range(shards)]
    )
    out_sum = reduce_shards(out_grads).astype(jnp.bfloat16)
    reduce_bits = [(0, 0)] + list(zip(first_order[::-1], second_order[::-1]))
    sum_bits = [0] + first_order

    def reduce_stage(up_grads, down_grads):
        up_bit, down_bit = reduce_bits.pop(0)
        return reduce_step(up_grads, up_bit), reduce_step(down_grads, down_bit)

    up_grads, down_grads = reduce_stage(up_grads, down_grads)
    grads = []
    for row in range(row_count):
        row_q, row_k, row_v, row_ctx, row_lse, low, high, bounds = rows[row]
        row_kt = row_k.T
        row_grad = d_context[row * seq_len : (row + 1) * seq_len]
        carried = None
        key_grads = []
        for part in range(parts):
            if row == 0 and part > 0:
                row_grad, (up_grads, down_grads, out_sum, own_sums) = tie(
                    row_grad, (up_grads, down_grads, out_sum, own_sums)
                )
                if part == min(2, parts - 1):
                    row_grad, output = tie(row_grad, output)
                if reduce_bits:
                    up_grads, down_grads = reduce_stage(up_grads, down_grads)
                if sum_bits:
                    bit = sum_bits.pop(0)
                    out_sum = add_low(out_sum, flip(out_sum, bit))
                    own_sums = add_low(own_sums, flip(own_sums, bit))
            carried, part_dk, part_dv = attend_backward(
                row_q, row_k, row_v, row_kt, row_grad, row_ctx, row_lse, low, high, bounds,
                part, parts, carried,
            )
            key_grads.append((part_dk, part_dv))
        grads.append(
            (
                carried,
                jnp.concatenate([item[0] for item in key_grads], axis=0),
                jnp.concatenate([item[1] for item in key_grads], axis=0),
            )
        )
    while reduce_bits:
        up_grads, down_grads = reduce_stage(up_grads, down_grads)
    for bit in sum_bits:
        out_sum = add_low(out_sum, flip(out_sum, bit))
        own_sums = add_low(own_sums, flip(own_sums, bit))
    grad_w_out = out_sum.astype(jnp.float32)
    piece_shape = (shards, piece_len, full_width)
    both_sum = jnp.stack(
        [up_grads[0].reshape(piece_shape), down_grads[0].reshape(piece_shape)], axis=1
    )
    own_piece = reduce_shards([both_sum[s] for s in range(shards)]).astype(jnp.bfloat16)
    all_pieces = {0: own_piece}
    for bit in first_order + [0]:
        all_pieces = gather_step(all_pieces, bit)
    grad_w_down = in_order(
        [all_pieces[j][1].astype(jnp.float32) for j in range(members)],
        (members, piece_len, full_width), 0, lambda j: member ^ j,
    ).reshape(w_down.shape)
    grad_w_up = in_order(
        [all_pieces[j][0].astype(jnp.float32).T for j in range(members)],
        (full_width, members, piece_len), 1, lambda j: member ^ j,
    ).reshape(w_up.shape)
    sums = [own_sums[i * slice_width : (i + 1) * slice_width] for i in range(6)]
    sum_b_up = own_sums[6 * slice_width : -3]
    totals_all = own_sums[-3:]
    lex_stats = jnp.stack([totals_all[1] / totals_all[0], totals_all[2] / totals_all[0]])

    d_queries, d_keys, d_values = (
        jnp.concatenate([item[i] for item in grads], axis=0) for i in range(3)
    )
    d_input_term = (
        inner_last(d_queries, w_query) + inner_last(d_keys, w_key) + inner_last(d_values, w_value)
    )
    own_shape = (row_count * parts, 1, own_len, full_width)
    split_term = d_input_term.reshape(row_count * parts, shards, own_len, full_width)
    mine = lax.broadcasted_iota(jnp.int32, (1, shards, 1, 1), 1) == me
    split_term = split_term + jnp.where(mine, d_first_res.reshape(own_shape), 0.0)
    d_input_term = split_term.astype(jnp.bfloat16).reshape(token_count, full_width)
    grad_inputs = lax.psum_scatter(d_input_term, "tensor", scatter_dimension=1, tiled=True)
    d_query_sum = sum_members(inner_first(flat, d_queries).astype(jnp.bfloat16), first_order)
    d_key_sum = sum_members(inner_first(flat, d_keys).astype(jnp.bfloat16), second_order)
    d_value_sum = sum_members(inner_first(flat, d_values).astype(jnp.bfloat16), first_order)
    bias_sums = sum_members(
        jnp.stack(
            [
                jnp.sum(d_queries, axis=0, dtype=jnp.float32),
                jnp.sum(d_values, axis=0, dtype=jnp.float32),
            ]
        ),
        first_order,
    )
    out_shape = (row_count, seq_len, slice_width)
    output = output.reshape(shards, row_count * parts, own_len, slice_width)
    output = output.transpose(1, 0, 2, 3)
    return (
        output.reshape(out_shape),
        grad_inputs.reshape(out_shape),
        d_query_sum.astype(jnp.float32),
        bias_sums[0],
        d_key_sum.astype(jnp.float32),
        d_value_sum.astype(jnp.float32),
        bias_sums[1],
        grad_w_out,
        sums[0],
        sums[1],
        sums[2],
        grad_w_up,
        sum_b_up,
        grad_w_down,
        sums[3],
        sums[4],
        sums[5],
        lex_stats,
    )


def solution(mesh):
    in_specs = (
        P("batch", None, None),
        P("batch", None),
        P("batch", None),
        P(None, "tensor"),
        P("tensor"),
        P(None, "tensor"),
        P(None, "tensor"),
        P("tensor"),
        P("tensor", None),
        P("tensor"),
        P("tensor"),
        P("tensor"),
        P(None, "tensor"),
        P("tensor"),
        P("tensor", None),
        P("tensor"),
        P("tensor"),
        P("tensor"),
        P("tensor"),
        P(),
        P("batch", None, "tensor"),
    )
    out_specs = (
        P("batch", None, "tensor"),
        P("batch", None, "tensor"),
        P(None, "tensor"),
        P("tensor"),
        P(None, "tensor"),
        P(None, "tensor"),
        P("tensor"),
        P("tensor", None),
        P("tensor"),
        P("tensor"),
        P("tensor"),
        P(None, "tensor"),
        P("tensor"),
        P("tensor", None),
        P("tensor"),
        P("tensor"),
        P("tensor"),
        P(),
    )
    return jax.shard_map(local, mesh=mesh, in_specs=in_specs, out_specs=out_specs, check_vma=False)
```

```python
import math, functools
import jax
import jax.numpy as jnp
from jax import lax
from jax.experimental import pallas as pl
from jax.experimental.pallas import tpu as pltpu

HEAD_DIM = 64
MASKED = -1e30
NT = (((1,), (1,)), ((), ()))
NN = (((1,), (0,)), ((), ()))


def dot_f32(left, right, dims):
    return lax.dot_general(left, right, dims, preferred_element_type=jnp.float32)


def head_lanes(shape, slot):
    lane = lax.broadcasted_iota(jnp.int32, shape, 1)
    return (lane >= slot * HEAD_DIM) & (lane < (slot + 1) * HEAD_DIM)


def pick_head(block, head, pair_width):
    group, slot = divmod(head * HEAD_DIM, pair_width)
    pair = block[:, group * pair_width : (group + 1) * pair_width]
    if pair_width == HEAD_DIM:
        return pair
    return jnp.where(head_lanes(pair.shape, slot // HEAD_DIM), pair, jnp.zeros_like(pair))


def allowed_tile(key_start, query_start, low_row, high_row, size):
    key_pos = key_start + lax.broadcasted_iota(jnp.int32, (size, 1), 0)
    query_pos = query_start + lax.broadcasted_iota(jnp.int32, (1, size), 1)
    return ((key_pos >= low_row) & (key_pos < high_row)) | (key_pos == query_pos)


def forward_body(
    first_block, size, heads, pair_width,
    bounds_ref, q_ref, k_ref, vt_ref, low_ref, high_ref,
    ctx_ref, lse_ref,
    qh_ref, acc_ref, max_ref, sum_ref,
):
    block = first_block + pl.program_id(0)
    for head in range(heads):
        qh_ref[head] = pick_head(q_ref[...], head, pair_width) * jnp.bfloat16(0.125)
    acc_ref[...] = jnp.zeros_like(acc_ref)
    max_ref[...] = jnp.full_like(max_ref, MASKED)
    sum_ref[...] = jnp.zeros_like(sum_ref)
    low_first, low_last = bounds_ref[0, block], bounds_ref[1, block]
    high_first, high_last = bounds_ref[2, block], bounds_ref[3, block]
    lower = low_first // size
    count = jnp.maximum((high_last + size - 1) // size - lower, 0)
    extra = jnp.where(block < lower + count, 0, 1)

    def visit(key_block, masked):
        key_start = pl.multiple_of(key_block * size, size)
        keys = pl.ds(key_start, size)
        if masked:
            allowed = allowed_tile(
                key_start, block * size, low_ref[...], high_ref[...], size
            )
        raw = []
        for head in range(heads):
            base = head * HEAD_DIM // pair_width * pair_width
            raw.append(dot_f32(k_ref[keys, base : base + pair_width], qh_ref[head], NT))
        old_max = [max_ref[head] for head in range(heads)]
        old_sum = [sum_ref[head] for head in range(heads)]
        new_max, new_sum, scales, low_expo = [], [], [], []
        for head in range(heads):
            scores = jnp.where(allowed, raw[head], MASKED) if masked else raw[head]
            top = jnp.maximum(old_max[head], jnp.max(scores, axis=0, keepdims=True))
            expo = jnp.exp(scores - top)
            scale = jnp.exp(old_max[head] - top)
            new_max.append(top)
            scales.append(scale)
            new_sum.append(old_sum[head] * scale + jnp.sum(expo, axis=0, keepdims=True))
            low_expo.append(expo.astype(jnp.bfloat16))
        terms = [
            dot_f32(vt_ref[head * HEAD_DIM : (head + 1) * HEAD_DIM, keys], low_expo[head], NN)
            for head in range(heads)
        ]
        for head in range(heads):
            rows = slice(head * HEAD_DIM, (head + 1) * HEAD_DIM)
            acc_ref[rows, :] = acc_ref[rows, :] * scales[head] + terms[head]
            max_ref[head] = new_max[head]
            sum_ref[head] = new_sum[head]

    def step(index, carry):
        key_block = jnp.where(index < count, lower + index, block)
        key_start = key_block * size
        full = (key_start >= low_last) & (key_start + size <= high_first)
        pl.when(full)(lambda: visit(key_block, False))
        pl.when(jnp.logical_not(full))(lambda: visit(key_block, True))
        return carry

    lax.fori_loop(0, count + extra, step, 0)
    for head in range(heads):
        rows = slice(head * HEAD_DIM, (head + 1) * HEAD_DIM)
        acc_ref[rows, :] = acc_ref[rows, :] / sum_ref[head]
        lse_ref[head : head + 1, :] = max_ref[head] + jnp.log(sum_ref[head])
    ctx_ref[...] = acc_ref[...].T.astype(jnp.bfloat16)


def block_size_of(tokens):
    return min(256, tokens)


def attend_forward(q, k, vt, low, high, bounds, first=0, last=None):
    tokens, width = q.shape
    size = block_size_of(tokens)
    heads = width // HEAD_DIM
    pair_width = min(128, width)
    last = tokens // size if last is None else last
    grid = last - first
    row_spec = pl.BlockSpec((1, size), lambda i, b: (0, i + first))
    return pl.pallas_call(
        functools.partial(forward_body, first, size, heads, pair_width),
        name="attend_forward",
        out_shape=(
            jax.ShapeDtypeStruct((grid * size, width), jnp.bfloat16),
            jax.ShapeDtypeStruct((heads, grid * size), jnp.float32),
        ),
        grid_spec=pltpu.PrefetchScalarGridSpec(
            num_scalar_prefetch=1,
            grid=(grid,),
            in_specs=[
                pl.BlockSpec((size, width), lambda i, b: (i + first, 0)),
                pl.BlockSpec((tokens, width), lambda i, b: (0, 0), pipeline_mode=pl.Buffered(1)),
                pl.BlockSpec((width, tokens), lambda i, b: (0, 0), pipeline_mode=pl.Buffered(1)),
                row_spec,
                row_spec,
            ],
            out_specs=[
                pl.BlockSpec((size, width), lambda i, b: (i, 0)),
                pl.BlockSpec((heads, size), lambda i, b: (0, i)),
            ],
            scratch_shapes=[
                pltpu.VMEM((heads, size, pair_width), jnp.bfloat16),
                pltpu.VMEM((width, size), jnp.float32),
                pltpu.VMEM((heads, 1, size), jnp.float32),
                pltpu.VMEM((heads, 1, size), jnp.float32),
            ],
        ),
        compiler_params=pltpu.CompilerParams(vmem_limit_bytes=40 << 20),
        cost_estimate=pl.CostEstimate(
            flops=8 * grid * size * tokens * width, transcendentals=0, bytes_accessed=6 * tokens * width
        ),
    )(bounds, q, k, vt, low, high)


def backward_body(
    first_block, is_first, is_last, size, heads, pair_width, all_blocks,
    bounds_ref, q_ref, k_ref, v_ref, kt_ref, do_ref, ctx_ref, lse_ref, low_ref, high_ref,
    *refs,
):
    carried_ref = None if is_first else refs[0]
    dq_ref, dk_ref, dv_ref, qh_ref, doh_ref, delta_ref = refs[0 if is_first else 1 :][:6]
    dk_acc, dv_acc = refs[-2:]
    dqt_ref = refs[-3] if is_last else dq_ref
    step_index = pl.program_id(0)
    block = first_block + step_index

    @pl.when(step_index == 0)
    def _():
        dqt_ref[...] = jnp.zeros_like(dqt_ref) if is_first else carried_ref[...]

        def prepare(index, carry):
            rows = pl.ds(pl.multiple_of(index * size, size), size)
            for head in range(heads):
                qh_ref[head, rows, :] = pick_head(q_ref[rows, :], head, pair_width) * jnp.bfloat16(0.125)
                doh_ref[head, rows, :] = pick_head(do_ref[rows, :], head, pair_width)
            both = (do_ref[rows, :].astype(jnp.float32) * ctx_ref[rows, :].astype(jnp.float32)).T
            for head in range(heads):
                part = both[head * HEAD_DIM : (head + 1) * HEAD_DIM, :]
                delta_ref[head, :, rows] = jnp.sum(part, axis=0, keepdims=True)
            return carry

        lax.fori_loop(0, all_blocks, prepare, 0)

    dk_acc[...] = jnp.zeros_like(dk_acc)
    dv_acc[...] = jnp.zeros_like(dv_acc)
    key_start = block * size
    lower, upper = bounds_ref[4, block], bounds_ref[5, block]

    def visit(query_block, masked):
        query_start = pl.multiple_of(query_block * size, size)
        rows = pl.ds(query_start, size)
        if masked:
            allowed = allowed_tile(
                key_start, query_start, low_ref[:, rows], high_ref[:, rows], size
            )
        spans = []
        for head in range(heads):
            group = head * HEAD_DIM // pair_width
            spans.append(slice(group * pair_width, (group + 1) * pair_width))
        every = range(heads)
        queries = [qh_ref[head, rows, :] for head in every]
        grads = [doh_ref[head, rows, :] for head in every]
        scores = [dot_f32(k_ref[:, spans[head]], queries[head], NT) for head in every]
        d_weights = [dot_f32(v_ref[:, spans[head]], grads[head], NT) for head in every]
        low_weights, d_scores = [], []
        for head in every:
            weights = jnp.exp(scores[head] - lse_ref[head : head + 1, rows])
            if masked:
                weights = jnp.where(allowed, weights, 0.0)
            low_weights.append(weights.astype(jnp.bfloat16))
            d_scores.append(
                (weights * (d_weights[head] - delta_ref[head, :, rows])).astype(jnp.bfloat16)
            )
        for lanes in sorted(set((span.start, span.stop) for span in spans)):
            span = slice(*lanes)
            mates = [head for head in every if spans[head] == span]
            dv_acc[:, span] += sum(dot_f32(low_weights[head], grads[head], NN) for head in mates)
            dk_acc[:, span] += sum(dot_f32(d_scores[head], queries[head], NN) for head in mates)
        turned = [
            dot_f32(kt_ref[head * HEAD_DIM : (head + 1) * HEAD_DIM, :], d_scores[head], NN)
            for head in every
        ]
        for head in every:
            dqt_ref[head * HEAD_DIM : (head + 1) * HEAD_DIM, rows] += turned[head]

    def step(query_block, carry):
        full = (key_start >= bounds_ref[1, query_block]) & (
            key_start + size <= bounds_ref[2, query_block]
        )
        pl.when(full)(lambda: visit(query_block, False))
        pl.when(jnp.logical_not(full))(lambda: visit(query_block, True))
        return carry

    lax.fori_loop(lower, upper, step, 0)
    dk_ref[...] = dk_acc[...].astype(jnp.bfloat16)
    dv_ref[...] = dv_acc[...].astype(jnp.bfloat16)

    if is_last:

        @pl.when(step_index == pl.num_programs(0) - 1)
        def _():
            def finish(index, carry):
                rows = pl.ds(pl.multiple_of(index * size, size), size)
                dq_ref[rows, :] = (dqt_ref[:, rows] * 0.125).T.astype(jnp.bfloat16)
                return carry

            lax.fori_loop(0, all_blocks, finish, 0)


def attend_backward(q, k, v, kt, d_ctx, ctx, lse, low, high, bounds, part, parts, carried):
    tokens, width = q.shape
    size = block_size_of(tokens)
    heads = width // HEAD_DIM
    pair_width = min(128, width)
    all_blocks = tokens // size
    grid = all_blocks // parts
    first = part * grid
    is_first, is_last = part == 0, part == parts - 1
    once = pl.Buffered(1)
    whole = pl.BlockSpec((tokens, width), lambda i, b: (0, 0), pipeline_mode=once)
    turned = pl.BlockSpec((width, tokens), lambda i, b: (0, 0), pipeline_mode=once)
    block = pl.BlockSpec((size, width), lambda i, b: (i + first, 0))
    block_out = pl.BlockSpec((size, width), lambda i, b: (i, 0))
    row = pl.BlockSpec((1, tokens), lambda i, b: (0, 0), pipeline_mode=once)
    part_shape = jax.ShapeDtypeStruct((grid * size, width), jnp.bfloat16)
    query_grad = (
        jax.ShapeDtypeStruct((tokens, width), jnp.bfloat16)
        if is_last
        else jax.ShapeDtypeStruct((width, tokens), jnp.float32)
    )
    scratch = [
        pltpu.VMEM((heads, tokens, pair_width), jnp.bfloat16),
        pltpu.VMEM((heads, tokens, pair_width), jnp.bfloat16),
        pltpu.VMEM((heads, 1, tokens), jnp.float32),
    ]
    if is_last:
        scratch.append(pltpu.VMEM((width, tokens), jnp.float32))
    scratch += [pltpu.VMEM((size, width), jnp.float32)] * 2
    operands = [bounds, q, k, v, kt, d_ctx, ctx, lse, low, high]
    in_specs = [
        whole, block, block,
        pl.BlockSpec((width, size), lambda i, b: (0, i + first)),
        whole, whole,
        pl.BlockSpec((heads, tokens), lambda i, b: (0, 0), pipeline_mode=once),
        row, row,
    ]
    if not is_first:
        operands.append(carried)
        in_specs.append(turned)
    return pl.pallas_call(
        functools.partial(
            backward_body, first, is_first, is_last, size, heads, pair_width, all_blocks
        ),
        name="attend_backward",
        out_shape=[query_grad, part_shape, part_shape],
        grid_spec=pltpu.PrefetchScalarGridSpec(
            num_scalar_prefetch=1,
            grid=(grid,),
            in_specs=in_specs,
            out_specs=[whole if is_last else turned, block_out, block_out],
            scratch_shapes=scratch,
        ),
        compiler_params=pltpu.CompilerParams(vmem_limit_bytes=48 << 20),
        cost_estimate=pl.CostEstimate(
            flops=20 * grid * size * tokens * width, transcendentals=0, bytes_accessed=20 * tokens * width
        ),
    )(*operands)


def key_bounds(seg_row, valid_row, size):
    tokens = seg_row.shape[0]
    ids = jnp.arange(8, dtype=jnp.int32)
    starts = jnp.sum((seg_row[None, :] < ids[:, None]).astype(jnp.int32), axis=1)
    ends = jnp.sum((seg_row[None, :] <= ids[:, None]).astype(jnp.int32), axis=1)
    valid_count = jnp.sum(valid_row)
    member = seg_row[None, :] == ids[:, None]
    low = jnp.sum(jnp.where(member, starts[:, None], 0), axis=0)
    end = jnp.sum(jnp.where(member, ends[:, None], 0), axis=0)
    high = jnp.minimum(end, valid_count)
    first_key = jnp.arange(0, tokens, size, dtype=jnp.int32)
    own = first_key // size
    live = first_key < valid_count
    seg_blocks = seg_row.reshape(-1, size)
    last_live = jnp.minimum(first_key + size, valid_count) - 1
    last_text = jnp.sum((starts[None, :] <= last_live[:, None]).astype(jnp.int32), axis=1) - 1
    last_end = jnp.sum(jnp.where(last_text[:, None] == ids[None, :], ends[None, :], 0), axis=1)
    low_blocks, high_blocks = low.reshape(-1, size), high.reshape(-1, size)
    query_from = jnp.where(live, low_blocks[:, 0] // size, own)
    query_to = jnp.where(live, jnp.maximum((last_end + size - 1) // size, own + 1), own + 1)
    bounds = jnp.stack(
        [low_blocks[:, 0], low_blocks[:, -1], high_blocks[:, 0], high_blocks[:, -1], query_from, query_to]
    )
    return low[None, :], high[None, :], bounds


from jax.sharding import PartitionSpec as P

EPSILON = 1e-05
PARTS = 4


def inner_first(left, right):
    return dot_f32(left, right, (((0,), (0,)), ((), ())))


def inner_last(left, right):
    return dot_f32(left, right, NT)


def gelu_exact(value):
    return 0.5 * value * (1.0 + lax.erf(value * (1.0 / math.sqrt(2.0))))


def norm_stats(value):
    mean_value = jnp.mean(value, axis=1, keepdims=True)
    spread = jnp.mean(value * value, axis=1, keepdims=True) - mean_value * mean_value
    return mean_value, lax.rsqrt(spread + EPSILON)


def norm_backward(d_scaled, normed, scale):
    return scale * (
        d_scaled
        - jnp.mean(d_scaled, axis=1, keepdims=True)
        - normed * jnp.mean(d_scaled * normed, axis=1, keepdims=True)
    )


def flip(value, bit):
    members = lax.axis_size("batch")
    return lax.ppermute(value, "batch", [(i, i ^ (1 << bit)) for i in range(members)])


def shift(value, step):
    shards = lax.axis_size("tensor")
    return lax.ppermute(value, "tensor", [(i, (i + step) % shards) for i in range(shards)])


def heads_to_tokens(value):
    return lax.all_to_all(value, "tensor", split_axis=0, concat_axis=1, tiled=True)


def tokens_to_heads(value):
    return lax.all_to_all(value, "tensor", split_axis=1, concat_axis=0, tiled=True)


def bit_orders():
    bits = list(range(1, lax.axis_size("batch").bit_length() - 1))
    return bits, bits[::-1]


def tie(value, others):
    return lax.optimization_barrier((value, others))


def gather_step(chunks, bit):
    moved = {j | (1 << bit): flip(chunk, bit) for j, chunk in chunks.items()}
    return {**chunks, **moved}


def reduce_send(chunks, bit):
    return {j: flip(chunk, bit) for j, chunk in chunks.items() if j >> bit & 1}


def reduce_add(chunks, moved, bit):
    return {
        j: add_low(chunk, moved[j | (1 << bit)]) for j, chunk in chunks.items() if not j >> bit & 1
    }


def add_low(left, right):
    return (left.astype(jnp.float32) + right.astype(jnp.float32)).astype(left.dtype)


def sum_members(value, order):
    for bit in [0] + order:
        value = add_low(value, flip(value, bit))
    return value


def gather_shards(piece):
    return [piece] + [shift(piece, s) for s in range(1, lax.axis_size("tensor"))]


def reduce_shards(blocks):
    total = blocks[0].astype(jnp.float32)
    for s in range(1, len(blocks)):
        total = total + shift(blocks[s], -s).astype(jnp.float32)
    return total


def in_order(blocks, buffer_shape, axis, index_of):
    result = jnp.zeros(buffer_shape, blocks[0].dtype)
    for s, block in enumerate(blocks):
        result = lax.dynamic_update_slice_in_dim(
            result, jnp.expand_dims(block, axis), index_of(s), axis
        )
    return result


def local(
    inputs,
    segments,
    valid,
    w_query,
    b_query,
    w_key,
    w_value,
    b_value,
    w_out,
    b_out,
    gain_one,
    shift_one,
    w_up,
    b_up,
    w_down,
    b_down,
    gain_two,
    shift_two,
    lex_weight,
    lex_bias,
    cotangent,
):
    row_count, seq_len, full_width = inputs.shape
    token_count = row_count * seq_len
    shards = lax.axis_size("tensor")
    members = lax.axis_size("batch")
    me = lax.axis_index("tensor")
    local_width = w_query.shape[1]
    slice_width = full_width // shards
    own_count = token_count // shards
    flat = inputs.reshape(token_count, full_width)
    size = block_size_of(seq_len)

    parts = PARTS if seq_len % (PARTS * shards * 8) == 0 else 1
    part_len = seq_len // parts
    own_len = part_len // shards
    first_order, second_order = bit_orders()
    member = lax.axis_index("batch")
    piece_len = w_down.shape[0] // members

    def own_tokens(value):
        split = value.reshape((row_count * parts, shards, own_len) + value.shape[1:])
        picked = lax.dynamic_index_in_dim(split, me, 1, False)
        return picked.reshape((own_count,) + value.shape[1:])

    small = jnp.concatenate(
        [b_out, gain_one, shift_one, b_down, gain_two, shift_two, lex_weight, b_up]
    )
    small_all = in_order(
        gather_shards(small), (shards,) + small.shape, 0, lambda s: (me - s) % shards
    ).astype(jnp.float32)
    vectors = [
        small_all[:, i * slice_width : (i + 1) * slice_width].reshape(1, full_width)
        for i in range(7)
    ]
    b_out_v, gain_one_v, shift_one_v, b_down_v, gain_two_v, shift_two_v, lex_v = vectors

    def relative_order(value):
        turned = jnp.concatenate([value[:1], value[:0:-1]], axis=0)
        value = lax.dynamic_slice_in_dim(
            jnp.concatenate([turned, turned], axis=0), shards - me, shards, 0
        )
        rest = value.shape[2:]
        for bit in range(members.bit_length() - 1):
            split = value.reshape((shards, members >> (bit + 1), 2, 1 << bit) + rest)
            value = jnp.where((member >> bit) & 1 == 1, split[:, :, ::-1], split)
        return value.reshape((shards, members) + rest)

    b_up_all = small_all[:, 7 * slice_width :].reshape(shards, members, piece_len)
    b_up_all = relative_order(b_up_all)

    up_piece = lax.dynamic_slice_in_dim(w_up, member * piece_len, piece_len, 1).T
    down_piece = lax.dynamic_slice_in_dim(w_down, member * piece_len, piece_len, 0)
    both = gather_shards(jnp.stack([up_piece, down_piece]))
    out_blocks = gather_shards(w_out)
    up_chunks = {0: jnp.concatenate([item[0] for item in both], axis=0)}
    down_chunks = {0: jnp.concatenate([item[1] for item in both], axis=0)}
    gather_bits = list(zip(first_order, second_order)) + [(0, 0)]

    queries = (jnp.dot(flat, w_query, preferred_element_type=jnp.float32) + b_query).astype(
        jnp.bfloat16
    )
    key_rows = jnp.dot(flat, w_key, preferred_element_type=jnp.float32).astype(jnp.bfloat16)
    value_rows = (jnp.dot(flat, w_value, preferred_element_type=jnp.float32) + b_value).astype(
        jnp.bfloat16
    )
    split_cot = cotangent.reshape(row_count * parts, shards, own_len, slice_width)
    split_cot = split_cot.transpose(1, 0, 2, 3).reshape(token_count, slice_width)
    split_cot, (up_chunks, down_chunks, out_blocks) = tie(
        split_cot, (up_chunks, down_chunks, out_blocks)
    )
    d_final = heads_to_tokens(split_cot)
    rows = []
    arrived = []
    for row in range(row_count):
        span = slice(row * seq_len, (row + 1) * seq_len)
        low, high, bounds = key_bounds(segments[row], valid[row], size)
        row_q, row_k, row_v = queries[span], key_rows[span], value_rows[span]
        row_vt = row_v.T
        pieces = []
        for part in range(parts):
            if row == 0 and part > 0:
                row_q, (up_chunks, down_chunks) = tie(row_q, (up_chunks, down_chunks))
                if part == parts - 1:
                    row_q, d_final = tie(row_q, d_final)
                if part > 1:
                    row_q, arrived[part - 2] = tie(row_q, arrived[part - 2])
                if gather_bits:
                    up_bit, down_bit = gather_bits.pop(0)
                    up_chunks = gather_step(up_chunks, up_bit)
                    down_chunks = gather_step(down_chunks, down_bit)
            part_blocks = part_len // size
            piece = attend_forward(
                row_q, row_k, row_vt, low, high, bounds,
                part * part_blocks, (part + 1) * part_blocks,
            )
            pieces.append(piece)
            sent = piece[0].reshape(shards, own_len, local_width)
            slots = [lax.dynamic_index_in_dim(sent, me, 0, False)]
            for s in range(1, shards):
                slots.append(
                    shift(lax.dynamic_index_in_dim(sent, (me + s) % shards, 0, False), s)
                )
            arrived.append(slots)
        row_ctx = jnp.concatenate([item[0] for item in pieces], axis=0)
        row_lse = jnp.concatenate([item[1] for item in pieces], axis=1)
        rows.append((row_q, row_k, row_v, row_ctx, row_lse, low, high, bounds))
    for up_bit, down_bit in gather_bits:
        up_chunks = gather_step(up_chunks, up_bit)
        down_chunks = gather_step(down_chunks, down_bit)
    up_full = jnp.concatenate([up_chunks[j] for j in range(members)], axis=0)
    down_full = jnp.concatenate([down_chunks[j] for j in range(members)], axis=0)
    d_final = d_final.astype(jnp.float32)
    token_ctx = [jnp.concatenate([item[s] for item in arrived], axis=0) for s in range(shards)]

    first_res = own_tokens(flat).astype(jnp.float32) + b_out_v
    for left, right in zip(token_ctx, out_blocks):
        first_res = first_res + dot_f32(left, right, NN)
    mean_one, scale_one = norm_stats(first_res)
    normed_one = (first_res - mean_one) * scale_one
    first_out = normed_one * gain_one_v + shift_one_v
    first_low = first_out.astype(jnp.bfloat16)
    b_up_v = b_up_all.transpose(1, 0, 2).reshape(1, -1)
    pre_up = inner_last(first_low, up_full) + b_up_v
    hidden = gelu_exact(pre_up).astype(jnp.bfloat16)
    second_res = first_out + jnp.dot(hidden, down_full, preferred_element_type=jnp.float32) + b_down_v
    mean_two, scale_two = norm_stats(second_res)
    normed_two = (second_res - mean_two) * scale_two
    final_out = normed_two * gain_two_v + shift_two_v
    output = final_out.astype(jnp.bfloat16)
    lex_pre = jnp.sum(final_out * lex_v, axis=1) + lex_bias[0].astype(jnp.float32)
    valid_float = own_tokens(valid.reshape(token_count)).astype(jnp.float32)
    lex_totals = jnp.stack(
        [
            jnp.sum(valid_float),
            jnp.sum(jnp.maximum(lex_pre, 0.0) * valid_float),
            jnp.sum(jnp.where(lex_pre > 0.0, valid_float, 0.0)),
        ]
    )

    grad_gain_two = jnp.sum(d_final * normed_two, axis=0)
    grad_shift_two = jnp.sum(d_final, axis=0)
    d_second = norm_backward(d_final * gain_two_v, normed_two, scale_two)
    grad_b_down = jnp.sum(d_second, axis=0)
    d_ffn_low = d_second.astype(jnp.bfloat16)
    d_hidden = inner_last(d_ffn_low, down_full)
    _, gelu_back = jax.vjp(gelu_exact, pre_up)
    d_pre_up = gelu_back(d_hidden)[0].astype(jnp.bfloat16)
    d_first = d_second + jnp.dot(d_pre_up, up_full, preferred_element_type=jnp.float32)
    grad_b_up = jnp.sum(d_pre_up, axis=0, dtype=jnp.float32)
    grad_b_up = grad_b_up.reshape(members, shards, piece_len).transpose(1, 0, 2)
    grad_b_up = relative_order(grad_b_up)
    grad_gain_one = jnp.sum(d_first * normed_one, axis=0)
    grad_shift_one = jnp.sum(d_first, axis=0)
    d_first_res = norm_backward(d_first * gain_one_v, normed_one, scale_one)
    grad_b_out = jnp.sum(d_first_res, axis=0)
    d_attn_low = d_first_res.astype(jnp.bfloat16)
    terms = [inner_last(d_attn_low, block).astype(jnp.bfloat16) for block in out_blocks]
    back = [term if s == 0 else shift(term, -s) for s, term in enumerate(terms)]
    def weight_grad(left, right):
        return inner_first(left, right).astype(jnp.bfloat16)

    chunk_len = shards * piece_len
    spans = [slice(j * chunk_len, (j + 1) * chunk_len) for j in range(members)]
    down_grads, up_grads, out_grads = {}, {}, []
    late = (hidden, d_pre_up, d_ffn_low, first_low)
    late, terms = tie(late, terms)
    groups = max(1, shards - 1)
    for group in range(groups):
        if group > 0:
            late, back[group] = tie(late, back[group])
        for index in range(group * 2 * members // groups, (group + 1) * 2 * members // groups):
            j = members - 1 - index // 2
            if index % 2 == 0:
                down_grads[j] = weight_grad(late[0][:, spans[j]], late[2])
            else:
                up_grads[j] = weight_grad(late[1][:, spans[j]], late[3])
    out_grads = [weight_grad(item, d_attn_low) for item in token_ctx]
    d_context = in_order(
        [item.reshape(row_count * parts, own_len, local_width) for item in back],
        (row_count * parts, shards, own_len, local_width),
        1,
        lambda s: (me + s) % shards,
    ).reshape(token_count, local_width)
    d_context, (down_grads, up_grads, out_grads) = tie(
        d_context, (down_grads, up_grads, out_grads)
    )
    token_sums = jnp.concatenate(
        [
            item.reshape(shards, -1)
            for item in (
                grad_b_out,
                grad_gain_one,
                grad_shift_one,
                grad_b_down,
                grad_gain_two,
                grad_shift_two,
                grad_b_up,
                jnp.broadcast_to(lex_totals, (shards, 3)),
            )
        ],
        axis=1,
    )
    own_sums = [
        lax.dynamic_index_in_dim(token_sums, (me - s) % shards, 0, False) for s in range(shards)
    ]
    reduce_bits = [(0, 0)] + list(zip(first_order[::-1], second_order[::-1]))
    sum_bits = [0] + first_order
    piece_shape = (shards, piece_len, full_width)

    class Stages:
        def __init__(self):
            self.at = 0
            self.up, self.down, self.out, self.small = up_grads, down_grads, out_grads, own_sums
            self.piece = None

        def send(self):
            at = self.at
            self.moved = [None] * 3
            if at < len(reduce_bits):
                up_bit, down_bit = reduce_bits[at]
                self.moved[0] = (reduce_send(self.up, up_bit), reduce_send(self.down, down_bit))
            elif at == len(reduce_bits):
                both_sum = jnp.stack(
                    [self.up[0].reshape(piece_shape), self.down[0].reshape(piece_shape)], axis=1
                )
                self.own_piece = both_sum[0]
                self.moved[0] = [shift(both_sum[s], -s) for s in range(1, shards)]
            if at == 0:
                self.moved[1] = [shift(self.out[s], -s) for s in range(1, shards)]
                self.moved[2] = [shift(self.small[s], -s) for s in range(1, shards)]
            elif at <= len(sum_bits):
                self.moved[1] = flip(self.out, sum_bits[at - 1])
                self.moved[2] = flip(self.small, sum_bits[at - 1])

        def add(self):
            at, moved = self.at, self.moved
            if at < len(reduce_bits):
                up_bit, down_bit = reduce_bits[at]
                self.up = reduce_add(self.up, moved[0][0], up_bit)
                self.down = reduce_add(self.down, moved[0][1], down_bit)
            elif at == len(reduce_bits):
                total = self.own_piece.astype(jnp.float32)
                for item in moved[0]:
                    total = total + item.astype(jnp.float32)
                self.piece = total.astype(jnp.bfloat16)
            if at == 0:
                total = self.out[0].astype(jnp.float32)
                for item in moved[1]:
                    total = total + item.astype(jnp.float32)
                self.out = total.astype(jnp.bfloat16)
                self.small = sum(moved[2], self.small[0])
            elif at <= len(sum_bits):
                self.out = add_low(self.out, moved[1])
                self.small = add_low(self.small, moved[2])
            self.at += 1

        def busy(self):
            return self.at <= max(len(reduce_bits), len(sum_bits))

    stages = Stages()
    grads = []
    for row in range(row_count):
        row_q, row_k, row_v, row_ctx, row_lse, low, high, bounds = rows[row]
        row_kt = row_k.T
        row_grad = d_context[row * seq_len : (row + 1) * seq_len]
        carried = None
        key_grads = []
        for part in range(parts):
            staged = row == 0 and stages.busy()
            if row == 0 and part == parts - 1:
                row_grad, output = tie(row_grad, output)
            if staged:
                stages.send()
            carried, part_dk, part_dv = attend_backward(
                row_q, row_k, row_v, row_kt, row_grad, row_ctx, row_lse, low, high, bounds,
                part, parts, carried,
            )
            if row == 0 and part == 0:
                (output, carried) = tie(output, carried)
                output = tokens_to_heads(output)
            if staged:
                stages.moved, part_dk = tie(stages.moved, part_dk)
                stages.add()
            key_grads.append((part_dk, part_dv))
        grads.append(
            (
                carried,
                jnp.concatenate([item[0] for item in key_grads], axis=0),
                jnp.concatenate([item[1] for item in key_grads], axis=0),
            )
        )
    while stages.busy():
        stages.send()
        stages.add()
    out_sum, own_sums, own_piece = stages.out, stages.small, stages.piece
    grad_w_out = out_sum.astype(jnp.float32)
    all_pieces = {0: own_piece}
    for bit in first_order + [0]:
        all_pieces = gather_step(all_pieces, bit)
    grad_w_down = in_order(
        [all_pieces[j][1].astype(jnp.float32) for j in range(members)],
        (members, piece_len, full_width), 0, lambda j: member ^ j,
    ).reshape(w_down.shape)
    grad_w_up = in_order(
        [all_pieces[j][0] for j in range(members)],
        (members, piece_len, full_width), 0, lambda j: member ^ j,
    ).reshape(w_up.shape[::-1]).astype(jnp.float32).T
    sums = [own_sums[i * slice_width : (i + 1) * slice_width] for i in range(6)]
    sum_b_up = own_sums[6 * slice_width : -3]
    totals_all = own_sums[-3:]
    lex_stats = jnp.stack([totals_all[1] / totals_all[0], totals_all[2] / totals_all[0]])

    d_queries, d_keys, d_values = (
        jnp.concatenate([item[i] for item in grads], axis=0) for i in range(3)
    )
    d_input_term = (
        inner_last(d_queries, w_query) + inner_last(d_keys, w_key) + inner_last(d_values, w_value)
    )
    own_shape = (row_count * parts, 1, own_len, full_width)
    split_term = d_input_term.reshape(row_count * parts, shards, own_len, full_width)
    mine = lax.broadcasted_iota(jnp.int32, (1, shards, 1, 1), 1) == me
    split_term = split_term + jnp.where(mine, d_first_res.reshape(own_shape), 0.0)
    d_input_term = split_term.astype(jnp.bfloat16).reshape(token_count, full_width)
    grad_inputs = lax.psum_scatter(d_input_term, "tensor", scatter_dimension=1, tiled=True)
    d_query_sum = sum_members(inner_first(flat, d_queries).astype(jnp.bfloat16), first_order)
    d_key_sum = sum_members(inner_first(flat, d_keys).astype(jnp.bfloat16), second_order)
    d_value_sum = sum_members(inner_first(flat, d_values).astype(jnp.bfloat16), first_order)
    bias_sums = sum_members(
        jnp.stack(
            [
                jnp.sum(d_queries, axis=0, dtype=jnp.float32),
                jnp.sum(d_values, axis=0, dtype=jnp.float32),
            ]
        ),
        first_order,
    )
    out_shape = (row_count, seq_len, slice_width)
    output = output.reshape(shards, row_count * parts, own_len, slice_width)
    output = output.transpose(1, 0, 2, 3)
    return (
        output.reshape(out_shape),
        grad_inputs.reshape(out_shape),
        d_query_sum.astype(jnp.float32),
        bias_sums[0],
        d_key_sum.astype(jnp.float32),
        d_value_sum.astype(jnp.float32),
        bias_sums[1],
        grad_w_out,
        sums[0],
        sums[1],
        sums[2],
        grad_w_up,
        sum_b_up,
        grad_w_down,
        sums[3],
        sums[4],
        sums[5],
        lex_stats,
    )


def solution(mesh):
    in_specs = (
        P("batch", None, None),
        P("batch", None),
        P("batch", None),
        P(None, "tensor"),
        P("tensor"),
        P(None, "tensor"),
        P(None, "tensor"),
        P("tensor"),
        P("tensor", None),
        P("tensor"),
        P("tensor"),
        P("tensor"),
        P(None, "tensor"),
        P("tensor"),
        P("tensor", None),
        P("tensor"),
        P("tensor"),
        P("tensor"),
        P("tensor"),
        P(),
        P("batch", None, "tensor"),
    )
    out_specs = (
        P("batch", None, "tensor"),
        P("batch", None, "tensor"),
        P(None, "tensor"),
        P("tensor"),
        P(None, "tensor"),
        P(None, "tensor"),
        P("tensor"),
        P("tensor", None),
        P("tensor"),
        P("tensor"),
        P("tensor"),
        P(None, "tensor"),
        P("tensor"),
        P("tensor", None),
        P("tensor"),
        P("tensor"),
        P("tensor"),
        P(),
    )
    return jax.shard_map(local, mesh=mesh, in_specs=in_specs, out_specs=out_specs, check_vma=False)
```

```python
import math, functools
import jax
import jax.numpy as jnp
from jax import lax
from jax.experimental import pallas as pl
from jax.experimental.pallas import tpu as pltpu

HEAD_DIM = 64
MASKED = -1e30
NT = (((1,), (1,)), ((), ()))
NN = (((1,), (0,)), ((), ()))


def dot_f32(left, right, dims):
    return lax.dot_general(left, right, dims, preferred_element_type=jnp.float32)


def head_lanes(shape, slot):
    lane = lax.broadcasted_iota(jnp.int32, shape, 1)
    return (lane >= slot * HEAD_DIM) & (lane < (slot + 1) * HEAD_DIM)


def pick_head(block, head, pair_width):
    group, slot = divmod(head * HEAD_DIM, pair_width)
    pair = block[:, group * pair_width : (group + 1) * pair_width]
    if pair_width == HEAD_DIM:
        return pair
    return jnp.where(head_lanes(pair.shape, slot // HEAD_DIM), pair, jnp.zeros_like(pair))


def allowed_tile(key_start, query_start, low_row, high_row, size):
    key_pos = key_start + lax.broadcasted_iota(jnp.int32, (size, 1), 0)
    query_pos = query_start + lax.broadcasted_iota(jnp.int32, (1, size), 1)
    return ((key_pos >= low_row) & (key_pos < high_row)) | (key_pos == query_pos)


def forward_body(
    first_block, size, heads, pair_width,
    bounds_ref, q_ref, k_ref, vt_ref, low_ref, high_ref,
    ctx_ref, lse_ref,
    qh_ref, acc_ref, max_ref, sum_ref,
):
    block = first_block + pl.program_id(0)
    for head in range(heads):
        qh_ref[head] = pick_head(q_ref[...], head, pair_width) * jnp.bfloat16(0.125)
    acc_ref[...] = jnp.zeros_like(acc_ref)
    max_ref[...] = jnp.full_like(max_ref, MASKED)
    sum_ref[...] = jnp.zeros_like(sum_ref)
    low_first, low_last = bounds_ref[0, block], bounds_ref[1, block]
    high_first, high_last = bounds_ref[2, block], bounds_ref[3, block]
    lower = low_first // size
    count = jnp.maximum((high_last + size - 1) // size - lower, 0)
    extra = jnp.where(block < lower + count, 0, 1)

    def visit(key_block, masked):
        key_start = pl.multiple_of(key_block * size, size)
        keys = pl.ds(key_start, size)
        if masked:
            allowed = allowed_tile(
                key_start, block * size, low_ref[...], high_ref[...], size
            )
        raw = []
        for head in range(heads):
            base = head * HEAD_DIM // pair_width * pair_width
            raw.append(dot_f32(k_ref[keys, base : base + pair_width], qh_ref[head], NT))
        old_max = [max_ref[head] for head in range(heads)]
        old_sum = [sum_ref[head] for head in range(heads)]
        new_max, new_sum, scales, low_expo = [], [], [], []
        for head in range(heads):
            scores = jnp.where(allowed, raw[head], MASKED) if masked else raw[head]
            top = jnp.maximum(old_max[head], jnp.max(scores, axis=0, keepdims=True))
            expo = jnp.exp(scores - top)
            scale = jnp.exp(old_max[head] - top)
            new_max.append(top)
            scales.append(scale)
            new_sum.append(old_sum[head] * scale + jnp.sum(expo, axis=0, keepdims=True))
            low_expo.append(expo.astype(jnp.bfloat16))
        terms = [
            dot_f32(vt_ref[head * HEAD_DIM : (head + 1) * HEAD_DIM, keys], low_expo[head], NN)
            for head in range(heads)
        ]
        for head in range(heads):
            rows = slice(head * HEAD_DIM, (head + 1) * HEAD_DIM)
            acc_ref[rows, :] = acc_ref[rows, :] * scales[head] + terms[head]
            max_ref[head] = new_max[head]
            sum_ref[head] = new_sum[head]

    def step(index, carry):
        key_block = jnp.where(index < count, lower + index, block)
        key_start = key_block * size
        full = (key_start >= low_last) & (key_start + size <= high_first)
        pl.when(full)(lambda: visit(key_block, False))
        pl.when(jnp.logical_not(full))(lambda: visit(key_block, True))
        return carry

    lax.fori_loop(0, count + extra, step, 0)
    for head in range(heads):
        rows = slice(head * HEAD_DIM, (head + 1) * HEAD_DIM)
        acc_ref[rows, :] = acc_ref[rows, :] / sum_ref[head]
        lse_ref[head : head + 1, :] = max_ref[head] + jnp.log(sum_ref[head])
    ctx_ref[...] = acc_ref[...].T.astype(jnp.bfloat16)


def block_size_of(tokens):
    return min(256, tokens)


def attend_forward(q, k, vt, low, high, bounds, first=0, last=None):
    tokens, width = q.shape
    size = block_size_of(tokens)
    heads = width // HEAD_DIM
    pair_width = min(128, width)
    last = tokens // size if last is None else last
    grid = last - first
    row_spec = pl.BlockSpec((1, size), lambda i, b: (0, i + first))
    return pl.pallas_call(
        functools.partial(forward_body, first, size, heads, pair_width),
        name="attend_forward",
        out_shape=(
            jax.ShapeDtypeStruct((grid * size, width), jnp.bfloat16),
            jax.ShapeDtypeStruct((heads, grid * size), jnp.float32),
        ),
        grid_spec=pltpu.PrefetchScalarGridSpec(
            num_scalar_prefetch=1,
            grid=(grid,),
            in_specs=[
                pl.BlockSpec((size, width), lambda i, b: (i + first, 0)),
                pl.BlockSpec((tokens, width), lambda i, b: (0, 0), pipeline_mode=pl.Buffered(1)),
                pl.BlockSpec((width, tokens), lambda i, b: (0, 0), pipeline_mode=pl.Buffered(1)),
                row_spec,
                row_spec,
            ],
            out_specs=[
                pl.BlockSpec((size, width), lambda i, b: (i, 0)),
                pl.BlockSpec((heads, size), lambda i, b: (0, i)),
            ],
            scratch_shapes=[
                pltpu.VMEM((heads, size, pair_width), jnp.bfloat16),
                pltpu.VMEM((width, size), jnp.float32),
                pltpu.VMEM((heads, 1, size), jnp.float32),
                pltpu.VMEM((heads, 1, size), jnp.float32),
            ],
        ),
        compiler_params=pltpu.CompilerParams(vmem_limit_bytes=40 << 20),
        cost_estimate=pl.CostEstimate(
            flops=8 * grid * size * tokens * width, transcendentals=0, bytes_accessed=6 * tokens * width
        ),
    )(bounds, q, k, vt, low, high)


def backward_body(
    plan, heads, pair_width,
    bounds_ref, q_ref, k_ref, v_ref, kt_ref, do_ref, ctx_ref, lse_ref, low_ref, high_ref,
    *refs,
):
    size, part_blocks, first_block, later, carried_later = plan
    refs = list(refs)
    carried_dq, carried_dk, carried_dv = (refs.pop(0) for _ in range(3)) if carried_later else (None,) * 3
    dq_ref, dk_ref, dv_ref = (refs.pop(0) for _ in range(3))
    next_dq = refs.pop(0) if later else None
    qh_ref, doh_ref, delta_ref, dqt_ref, dk_acc, dv_acc = refs
    step_index = pl.program_id(0)
    block = first_block + step_index
    part_len = part_blocks * size
    origin = first_block * size

    @pl.when(step_index == 0)
    def _():
        dqt_ref[...] = jnp.zeros_like(dqt_ref)
        if carried_later:
            dqt_ref[:, : carried_later * part_len] = carried_dq[...]

        def prepare(index, carry):
            rows = pl.ds(pl.multiple_of(index * size, size), size)
            taken = pl.ds(pl.multiple_of(origin + index * size, size), size)
            for head in range(heads):
                qh_ref[head, rows, :] = pick_head(q_ref[taken, :], head, pair_width) * jnp.bfloat16(0.125)
                doh_ref[head, rows, :] = pick_head(do_ref[taken, :], head, pair_width)
            both = (do_ref[taken, :].astype(jnp.float32) * ctx_ref[taken, :].astype(jnp.float32)).T
            for head in range(heads):
                part = both[head * HEAD_DIM : (head + 1) * HEAD_DIM, :]
                delta_ref[head, :, rows] = jnp.sum(part, axis=0, keepdims=True)
            return carry

        lax.fori_loop(0, (1 + later) * part_blocks, prepare, 0)

    dk_acc[...] = jnp.zeros_like(dk_acc)
    dv_acc[...] = jnp.zeros_like(dv_acc)
    key_start = block * size
    if carried_later:

        @pl.when(step_index < carried_later * part_blocks)
        def _():
            dk_acc[...] = carried_dk[...]
            dv_acc[...] = carried_dv[...]

    lower = jnp.maximum(bounds_ref[4, block], first_block)
    upper = jnp.where(
        step_index < part_blocks,
        bounds_ref[5, block],
        jnp.minimum(bounds_ref[5, block], first_block + part_blocks),
    )

    def visit(query_block, masked):
        query_start = pl.multiple_of(query_block * size, size)
        taken = pl.ds(query_start, size)
        rows = pl.ds(pl.multiple_of(query_start - origin, size), size)
        if masked:
            allowed = allowed_tile(
                key_start, query_start, low_ref[:, taken], high_ref[:, taken], size
            )
        spans = []
        for head in range(heads):
            group = head * HEAD_DIM // pair_width
            spans.append(slice(group * pair_width, (group + 1) * pair_width))
        every = range(heads)
        queries = [qh_ref[head, rows, :] for head in every]
        grads = [doh_ref[head, rows, :] for head in every]
        scores = [dot_f32(k_ref[:, spans[head]], queries[head], NT) for head in every]
        d_weights = [dot_f32(v_ref[:, spans[head]], grads[head], NT) for head in every]
        low_weights, d_scores = [], []
        for head in every:
            weights = jnp.exp(scores[head] - lse_ref[head : head + 1, taken])
            if masked:
                weights = jnp.where(allowed, weights, 0.0)
            low_weights.append(weights.astype(jnp.bfloat16))
            d_scores.append(
                (weights * (d_weights[head] - delta_ref[head, :, rows])).astype(jnp.bfloat16)
            )
        for lanes in sorted(set((span.start, span.stop) for span in spans)):
            span = slice(*lanes)
            mates = [head for head in every if spans[head] == span]
            dv_acc[:, span] += sum(dot_f32(low_weights[head], grads[head], NN) for head in mates)
            dk_acc[:, span] += sum(dot_f32(d_scores[head], queries[head], NN) for head in mates)
        turned = [
            dot_f32(kt_ref[head * HEAD_DIM : (head + 1) * HEAD_DIM, :], d_scores[head], NN)
            for head in every
        ]
        for head in every:
            dqt_ref[head * HEAD_DIM : (head + 1) * HEAD_DIM, rows] += turned[head]

    def step(query_block, carry):
        full = (key_start >= bounds_ref[1, query_block]) & (
            key_start + size <= bounds_ref[2, query_block]
        )
        pl.when(full)(lambda: visit(query_block, False))
        pl.when(jnp.logical_not(full))(lambda: visit(query_block, True))
        return carry

    lax.fori_loop(lower, upper, step, 0)
    dk_ref[...] = dk_acc[...]
    dv_ref[...] = dv_acc[...]

    @pl.when(step_index == pl.num_programs(0) - 1)
    def _():
        def finish(index, carry):
            rows = pl.ds(pl.multiple_of(index * size, size), size)
            dq_ref[rows, :] = (dqt_ref[:, rows] * 0.125).T.astype(jnp.bfloat16)
            return carry

        lax.fori_loop(0, part_blocks, finish, 0)
        if later:
            next_dq[...] = dqt_ref[:, part_len:]


LONGEST_TEXT = 2048


def attend_backward(q, k, v, kt, d_ctx, ctx, lse, low, high, bounds, part, parts, carried):
    tokens, width = q.shape
    size = block_size_of(tokens)
    heads = width // HEAD_DIM
    pair_width = min(128, width)
    part_blocks = tokens // size // parts
    part_len = part_blocks * size
    reach = -(-(LONGEST_TEXT - 1) // part_len)
    later = min(reach, parts - 1 - part)
    carried_later = min(reach, parts - part) if part else 0
    first = part * part_blocks
    grid = (1 + later) * part_blocks
    window = grid * size
    once = pl.Buffered(1)
    fixed = lambda i, b: (0, 0)
    whole = pl.BlockSpec((tokens, width), fixed, pipeline_mode=once)
    block = pl.BlockSpec((size, width), lambda i, b: (i + first, 0))
    block_out = pl.BlockSpec((size, width), lambda i, b: (i, 0))
    row = pl.BlockSpec((1, tokens), fixed, pipeline_mode=once)
    operands = [bounds, q, k, v, kt, d_ctx, ctx, lse, low, high]
    in_specs = [
        whole, block, block,
        pl.BlockSpec((width, size), lambda i, b: (0, i + first)),
        whole, whole,
        pl.BlockSpec((heads, tokens), fixed, pipeline_mode=once),
        row, row,
    ]
    if carried_later:
        operands += list(carried)
        last = carried[1].shape[0] // size - 1
        came = pl.BlockSpec((size, width), lambda i, b: (jnp.minimum(i + part_blocks, last), 0))
        in_specs += [
            pl.BlockSpec((width, carried_later * part_len), fixed, pipeline_mode=once), came, came
        ]
    out_shape = [
        jax.ShapeDtypeStruct((part_len, width), jnp.bfloat16),
        jax.ShapeDtypeStruct((window, width), jnp.float32),
        jax.ShapeDtypeStruct((window, width), jnp.float32),
    ]
    out_specs = [pl.BlockSpec((part_len, width), fixed, pipeline_mode=once), block_out, block_out]
    if later:
        out_shape.append(jax.ShapeDtypeStruct((width, later * part_len), jnp.float32))
        out_specs.append(pl.BlockSpec((width, later * part_len), fixed, pipeline_mode=once))
    results = pl.pallas_call(
        functools.partial(
            backward_body, (size, part_blocks, first, later, carried_later), heads, pair_width
        ),
        name="attend_backward",
        out_shape=out_shape,
        grid_spec=pltpu.PrefetchScalarGridSpec(
            num_scalar_prefetch=1,
            grid=(grid,),
            in_specs=in_specs,
            out_specs=out_specs,
            scratch_shapes=[
                pltpu.VMEM((heads, window, pair_width), jnp.bfloat16),
                pltpu.VMEM((heads, window, pair_width), jnp.bfloat16),
                pltpu.VMEM((heads, 1, window), jnp.float32),
                pltpu.VMEM((width, window), jnp.float32),
                pltpu.VMEM((size, width), jnp.float32),
                pltpu.VMEM((size, width), jnp.float32),
            ],
        ),
        compiler_params=pltpu.CompilerParams(vmem_limit_bytes=48 << 20),
        cost_estimate=pl.CostEstimate(
            flops=20 * part_len * tokens * width, transcendentals=0, bytes_accessed=20 * tokens * width
        ),
    )(*operands)
    d_query, d_key, d_value = results[:3]
    final = (
        d_query, d_key[:part_len].astype(jnp.bfloat16), d_value[:part_len].astype(jnp.bfloat16)
    )
    return final, ((results[3], d_key, d_value) if later else None)


def place_body(members, piece_len, member_ref, *refs):
    pieces, (down_ref, up_ref, rows_ref) = refs[:members], refs[members:]
    for j in range(members):
        at = pl.multiple_of((member_ref[0] ^ j) * piece_len, piece_len)
        down_ref[pl.ds(at, piece_len), :] = pieces[j][1].astype(jnp.float32)
        rows_ref[pl.ds(at, piece_len), :] = pieces[j][0].astype(jnp.float32)
    up_ref[...] = rows_ref[...].T


def place_pieces(pieces, member):
    members = len(pieces)
    _, piece_len, width = pieces[0].shape
    rows = members * piece_len
    whole = lambda shape: pl.BlockSpec(shape, lambda i, b: (0,) * len(shape), pipeline_mode=pl.Buffered(1))
    return pl.pallas_call(
        functools.partial(place_body, members, piece_len),
        name="place_pieces",
        out_shape=[
            jax.ShapeDtypeStruct((rows, width), jnp.float32),
            jax.ShapeDtypeStruct((width, rows), jnp.float32),
        ],
        grid_spec=pltpu.PrefetchScalarGridSpec(
            num_scalar_prefetch=1,
            grid=(1,),
            in_specs=[whole(item.shape) for item in pieces],
            out_specs=[whole((rows, width)), whole((width, rows))],
            scratch_shapes=[pltpu.VMEM((rows, width), jnp.float32)],
        ),
        compiler_params=pltpu.CompilerParams(vmem_limit_bytes=32 << 20),
    )(member.reshape(1).astype(jnp.int32), *pieces)


def key_bounds(seg_row, valid_row, size):
    tokens = seg_row.shape[0]
    ids = jnp.arange(8, dtype=jnp.int32)
    starts = jnp.sum((seg_row[None, :] < ids[:, None]).astype(jnp.int32), axis=1)
    ends = jnp.sum((seg_row[None, :] <= ids[:, None]).astype(jnp.int32), axis=1)
    valid_count = jnp.sum(valid_row)
    member = seg_row[None, :] == ids[:, None]
    low = jnp.sum(jnp.where(member, starts[:, None], 0), axis=0)
    end = jnp.sum(jnp.where(member, ends[:, None], 0), axis=0)
    high = jnp.minimum(end, valid_count)
    first_key = jnp.arange(0, tokens, size, dtype=jnp.int32)
    own = first_key // size
    live = first_key < valid_count
    seg_blocks = seg_row.reshape(-1, size)
    last_live = jnp.minimum(first_key + size, valid_count) - 1
    last_text = jnp.sum((starts[None, :] <= last_live[:, None]).astype(jnp.int32), axis=1) - 1
    last_end = jnp.sum(jnp.where(last_text[:, None] == ids[None, :], ends[None, :], 0), axis=1)
    low_blocks, high_blocks = low.reshape(-1, size), high.reshape(-1, size)
    query_from = jnp.where(live, low_blocks[:, 0] // size, own)
    query_to = jnp.where(live, jnp.maximum((last_end + size - 1) // size, own + 1), own + 1)
    bounds = jnp.stack(
        [low_blocks[:, 0], low_blocks[:, -1], high_blocks[:, 0], high_blocks[:, -1], query_from, query_to]
    )
    return low[None, :], high[None, :], bounds


from jax.sharding import PartitionSpec as P

EPSILON = 1e-05
PARTS = 4


def inner_first(left, right):
    return dot_f32(left, right, (((0,), (0,)), ((), ())))


def inner_last(left, right):
    return dot_f32(left, right, NT)


def gelu_exact(value):
    return 0.5 * value * (1.0 + lax.erf(value * (1.0 / math.sqrt(2.0))))


def norm_stats(value):
    mean_value = jnp.mean(value, axis=1, keepdims=True)
    spread = jnp.mean(value * value, axis=1, keepdims=True) - mean_value * mean_value
    return mean_value, lax.rsqrt(spread + EPSILON)


def norm_backward(d_scaled, normed, scale):
    return scale * (
        d_scaled
        - jnp.mean(d_scaled, axis=1, keepdims=True)
        - normed * jnp.mean(d_scaled * normed, axis=1, keepdims=True)
    )


def flip(value, bit):
    members = lax.axis_size("batch")
    return lax.ppermute(value, "batch", [(i, i ^ (1 << bit)) for i in range(members)])


def shift(value, step):
    shards = lax.axis_size("tensor")
    return lax.ppermute(value, "tensor", [(i, (i + step) % shards) for i in range(shards)])


def heads_to_tokens(value):
    return lax.all_to_all(value, "tensor", split_axis=0, concat_axis=1, tiled=True)


def tokens_to_heads(value):
    return lax.all_to_all(value, "tensor", split_axis=1, concat_axis=0, tiled=True)


def bit_orders():
    bits = list(range(1, lax.axis_size("batch").bit_length() - 1))
    return bits, bits[::-1]


def tie(value, others):
    return lax.optimization_barrier((value, others))


def gather_step(chunks, bit):
    moved = {j | (1 << bit): flip(chunk, bit) for j, chunk in chunks.items()}
    return {**chunks, **moved}


def reduce_send(chunks, bit):
    return {j: flip(chunk, bit) for j, chunk in chunks.items() if j >> bit & 1}


def reduce_add(chunks, moved, bit):
    return {
        j: add_low(chunk, moved[j | (1 << bit)]) for j, chunk in chunks.items() if not j >> bit & 1
    }


def add_low(left, right):
    return (left.astype(jnp.float32) + right.astype(jnp.float32)).astype(left.dtype)


def sum_members(value, order):
    for bit in [0] + order:
        value = add_low(value, flip(value, bit))
    return value


def gather_shards(piece):
    return [piece] + [shift(piece, s) for s in range(1, lax.axis_size("tensor"))]


def reduce_shards(blocks):
    total = blocks[0].astype(jnp.float32)
    for s in range(1, len(blocks)):
        total = total + shift(blocks[s], -s).astype(jnp.float32)
    return total


def in_order(blocks, buffer_shape, axis, index_of):
    result = jnp.zeros(buffer_shape, blocks[0].dtype)
    for s, block in enumerate(blocks):
        result = lax.dynamic_update_slice_in_dim(
            result, jnp.expand_dims(block, axis), index_of(s), axis
        )
    return result


def local(
    inputs,
    segments,
    valid,
    w_query,
    b_query,
    w_key,
    w_value,
    b_value,
    w_out,
    b_out,
    gain_one,
    shift_one,
    w_up,
    b_up,
    w_down,
    b_down,
    gain_two,
    shift_two,
    lex_weight,
    lex_bias,
    cotangent,
):
    row_count, seq_len, full_width = inputs.shape
    token_count = row_count * seq_len
    shards = lax.axis_size("tensor")
    members = lax.axis_size("batch")
    me = lax.axis_index("tensor")
    local_width = w_query.shape[1]
    slice_width = full_width // shards
    own_count = token_count // shards
    flat = inputs.reshape(token_count, full_width)
    size = block_size_of(seq_len)

    parts = PARTS if seq_len % (PARTS * shards * 8) == 0 else 1
    part_len = seq_len // parts
    own_len = part_len // shards
    first_order, second_order = bit_orders()
    member = lax.axis_index("batch")
    piece_len = w_down.shape[0] // members

    def own_tokens(value):
        split = value.reshape((row_count * parts, shards, own_len) + value.shape[1:])
        picked = lax.dynamic_index_in_dim(split, me, 1, False)
        return picked.reshape((own_count,) + value.shape[1:])

    ratio = b_up.shape[0] // slice_width
    short = [b_out, gain_one, shift_one, b_down, gain_two, shift_two, lex_weight]
    short += [b_up[i * slice_width : (i + 1) * slice_width] for i in range(ratio)]
    line = lax.broadcasted_iota(jnp.int32, (len(short), slice_width), 0)
    small = jnp.zeros(line.shape, jnp.float32)
    for i, item in enumerate(short):
        small = jnp.where(line == i, item.astype(jnp.float32)[None, :], small)
    small = small.astype(jnp.bfloat16)
    small_all = in_order(
        gather_shards(small), (shards,) + small.shape, 0, lambda s: (me - s) % shards
    ).astype(jnp.float32)
    vectors = [
        small_all[:, i].reshape(1, full_width)
        for i in range(7)
    ]
    b_out_v, gain_one_v, shift_one_v, b_down_v, gain_two_v, shift_two_v, lex_v = vectors

    def relative_order(value):
        turned = jnp.concatenate([value[:1], value[:0:-1]], axis=0)
        value = lax.dynamic_slice_in_dim(
            jnp.concatenate([turned, turned], axis=0), shards - me, shards, 0
        )
        rest = value.shape[2:]
        for bit in range(members.bit_length() - 1):
            split = value.reshape((shards, members >> (bit + 1), 2, 1 << bit) + rest)
            value = jnp.where((member >> bit) & 1 == 1, split[:, :, ::-1], split)
        return value.reshape((shards, members) + rest)

    b_up_all = small_all[:, 7:].reshape(shards, members, piece_len)
    b_up_all = relative_order(b_up_all)

    up_piece = lax.dynamic_slice_in_dim(w_up, member * piece_len, piece_len, 1).T
    down_piece = lax.dynamic_slice_in_dim(w_down, member * piece_len, piece_len, 0)
    both = gather_shards(jnp.stack([up_piece, down_piece]))
    out_blocks = gather_shards(w_out)
    up_chunks = {0: jnp.concatenate([item[0] for item in both], axis=0)}
    down_chunks = {0: jnp.concatenate([item[1] for item in both], axis=0)}
    gather_bits = list(zip(first_order, second_order)) + [(0, 0)]

    queries = (jnp.dot(flat, w_query, preferred_element_type=jnp.float32) + b_query).astype(
        jnp.bfloat16
    )
    key_rows = jnp.dot(flat, w_key, preferred_element_type=jnp.float32).astype(jnp.bfloat16)
    value_rows = (jnp.dot(flat, w_value, preferred_element_type=jnp.float32) + b_value).astype(
        jnp.bfloat16
    )
    split_cot = cotangent.reshape(row_count * parts, shards, own_len, slice_width)
    split_cot = split_cot.transpose(1, 0, 2, 3).reshape(token_count, slice_width)
    split_cot, (up_chunks, down_chunks, out_blocks) = tie(
        split_cot, (up_chunks, down_chunks, out_blocks)
    )
    d_final = heads_to_tokens(split_cot)
    rows = []
    arrived = []
    for row in range(row_count):
        span = slice(row * seq_len, (row + 1) * seq_len)
        low, high, bounds = key_bounds(segments[row], valid[row], size)
        row_q, row_k, row_v = queries[span], key_rows[span], value_rows[span]
        row_vt = row_v.T
        pieces = []
        for part in range(parts):
            if row == 0 and part > 0:
                row_q, (up_chunks, down_chunks) = tie(row_q, (up_chunks, down_chunks))
                if part == parts - 1:
                    row_q, d_final = tie(row_q, d_final)
                if part > 1:
                    row_q, arrived[part - 2] = tie(row_q, arrived[part - 2])
                if gather_bits:
                    up_bit, down_bit = gather_bits.pop(0)
                    up_chunks = gather_step(up_chunks, up_bit)
                    down_chunks = gather_step(down_chunks, down_bit)
            part_blocks = part_len // size
            piece = attend_forward(
                row_q, row_k, row_vt, low, high, bounds,
                part * part_blocks, (part + 1) * part_blocks,
            )
            pieces.append(piece)
            sent = piece[0].reshape(shards, own_len, local_width)
            slots = [lax.dynamic_index_in_dim(sent, me, 0, False)]
            for s in range(1, shards):
                slots.append(
                    shift(lax.dynamic_index_in_dim(sent, (me + s) % shards, 0, False), s)
                )
            arrived.append(slots)
        row_ctx = jnp.concatenate([item[0] for item in pieces], axis=0)
        row_lse = jnp.concatenate([item[1] for item in pieces], axis=1)
        rows.append((row_q, row_k, row_v, row_ctx, row_lse, low, high, bounds))
    for up_bit, down_bit in gather_bits:
        up_chunks = gather_step(up_chunks, up_bit)
        down_chunks = gather_step(down_chunks, down_bit)
    up_full = jnp.concatenate([up_chunks[j] for j in range(members)], axis=0)
    down_full = jnp.concatenate([down_chunks[j] for j in range(members)], axis=0)
    d_final = d_final.astype(jnp.float32)
    token_ctx = [jnp.concatenate([item[s] for item in arrived], axis=0) for s in range(shards)]

    first_res = own_tokens(flat).astype(jnp.float32) + b_out_v
    for left, right in zip(token_ctx, out_blocks):
        first_res = first_res + dot_f32(left, right, NN)
    mean_one, scale_one = norm_stats(first_res)
    normed_one = (first_res - mean_one) * scale_one
    first_out = normed_one * gain_one_v + shift_one_v
    first_low = first_out.astype(jnp.bfloat16)
    b_up_v = b_up_all.transpose(1, 0, 2).reshape(1, -1)
    pre_up = inner_last(first_low, up_full) + b_up_v
    hidden = gelu_exact(pre_up).astype(jnp.bfloat16)
    second_res = first_out + jnp.dot(hidden, down_full, preferred_element_type=jnp.float32) + b_down_v
    mean_two, scale_two = norm_stats(second_res)
    normed_two = (second_res - mean_two) * scale_two
    final_out = normed_two * gain_two_v + shift_two_v
    output = final_out.astype(jnp.bfloat16)
    lex_pre = jnp.sum(final_out * lex_v, axis=1) + lex_bias[0].astype(jnp.float32)
    valid_float = own_tokens(valid.reshape(token_count)).astype(jnp.float32)
    lex_totals = jnp.stack(
        [
            jnp.sum(valid_float),
            jnp.sum(jnp.maximum(lex_pre, 0.0) * valid_float),
            jnp.sum(jnp.where(lex_pre > 0.0, valid_float, 0.0)),
        ]
    )

    grad_gain_two = jnp.sum(d_final * normed_two, axis=0)
    grad_shift_two = jnp.sum(d_final, axis=0)
    d_second = norm_backward(d_final * gain_two_v, normed_two, scale_two)
    grad_b_down = jnp.sum(d_second, axis=0)
    d_ffn_low = d_second.astype(jnp.bfloat16)
    d_hidden = inner_last(d_ffn_low, down_full)
    _, gelu_back = jax.vjp(gelu_exact, pre_up)
    d_pre_up = gelu_back(d_hidden)[0].astype(jnp.bfloat16)
    d_first = d_second + jnp.dot(d_pre_up, up_full, preferred_element_type=jnp.float32)
    grad_b_up = jnp.sum(d_pre_up, axis=0, dtype=jnp.float32)
    grad_b_up = grad_b_up.reshape(members, shards, piece_len).transpose(1, 0, 2)
    grad_b_up = relative_order(grad_b_up)
    grad_gain_one = jnp.sum(d_first * normed_one, axis=0)
    grad_shift_one = jnp.sum(d_first, axis=0)
    d_first_res = norm_backward(d_first * gain_one_v, normed_one, scale_one)
    grad_b_out = jnp.sum(d_first_res, axis=0)
    d_attn_low = d_first_res.astype(jnp.bfloat16)
    terms = [inner_last(d_attn_low, block).astype(jnp.bfloat16) for block in out_blocks]
    back = [term if s == 0 else shift(term, -s) for s, term in enumerate(terms)]
    def weight_grad(left, right):
        return inner_first(left, right).astype(jnp.bfloat16)

    chunk_len = shards * piece_len
    spans = [slice(j * chunk_len, (j + 1) * chunk_len) for j in range(members)]
    down_grads, up_grads, out_grads = {}, {}, []
    late = (hidden, d_pre_up, d_ffn_low, first_low)
    late, terms = tie(late, terms)
    groups = max(1, shards - 1)
    for group in range(groups):
        if group > 0:
            late, back[group] = tie(late, back[group])
        for index in range(group * 2 * members // groups, (group + 1) * 2 * members // groups):
            j = members - 1 - index // 2
            if index % 2 == 0:
                down_grads[j] = weight_grad(late[0][:, spans[j]], late[2])
            else:
                up_grads[j] = weight_grad(late[1][:, spans[j]], late[3])
    out_grads = [weight_grad(item, d_attn_low) for item in token_ctx]
    d_context = in_order(
        [item.reshape(row_count * parts, own_len, local_width) for item in back],
        (row_count * parts, shards, own_len, local_width),
        1,
        lambda s: (me + s) % shards,
    ).reshape(token_count, local_width)
    d_context, (down_grads, up_grads, out_grads) = tie(
        d_context, (down_grads, up_grads, out_grads)
    )
    token_sums = jnp.concatenate(
        [
            item.reshape(shards, -1)
            for item in (
                grad_b_out,
                grad_gain_one,
                grad_shift_one,
                grad_b_down,
                grad_gain_two,
                grad_shift_two,
                grad_b_up,
                jnp.broadcast_to(lex_totals, (shards, 3)),
            )
        ],
        axis=1,
    )
    own_sums = [
        lax.dynamic_index_in_dim(token_sums, (me - s) % shards, 0, False) for s in range(shards)
    ]
    reduce_bits = [(0, 0)] + list(zip(first_order[::-1], second_order[::-1]))
    sum_bits = [0] + first_order
    piece_shape = (shards, piece_len, full_width)

    class Stages:
        def __init__(self):
            self.at = 0
            self.up, self.down, self.out, self.small = up_grads, down_grads, out_grads, own_sums
            self.piece = None

        def send(self):
            at = self.at
            self.moved = [None] * 3
            if at < len(reduce_bits):
                up_bit, down_bit = reduce_bits[at]
                self.moved[0] = (reduce_send(self.up, up_bit), reduce_send(self.down, down_bit))
            elif at == len(reduce_bits):
                both_sum = jnp.stack(
                    [self.up[0].reshape(piece_shape), self.down[0].reshape(piece_shape)], axis=1
                )
                self.own_piece = both_sum[0]
                self.moved[0] = [shift(both_sum[s], -s) for s in range(1, shards)]
            if at == 0:
                self.moved[1] = [shift(self.out[s], -s) for s in range(1, shards)]
                self.moved[2] = [shift(self.small[s], -s) for s in range(1, shards)]
            elif at <= len(sum_bits):
                self.moved[1] = flip(self.out, sum_bits[at - 1])
                self.moved[2] = flip(self.small, sum_bits[at - 1])

        def add(self):
            at, moved = self.at, self.moved
            if at < len(reduce_bits):
                up_bit, down_bit = reduce_bits[at]
                self.up = reduce_add(self.up, moved[0][0], up_bit)
                self.down = reduce_add(self.down, moved[0][1], down_bit)
            elif at == len(reduce_bits):
                total = self.own_piece.astype(jnp.float32)
                for item in moved[0]:
                    total = total + item.astype(jnp.float32)
                self.piece = total.astype(jnp.bfloat16)
            if at == 0:
                total = self.out[0].astype(jnp.float32)
                for item in moved[1]:
                    total = total + item.astype(jnp.float32)
                self.out = total.astype(jnp.bfloat16)
                self.small = sum(moved[2], self.small[0])
            elif at <= len(sum_bits):
                self.out = add_low(self.out, moved[1])
                self.small = add_low(self.small, moved[2])
            self.at += 1

        def busy(self):
            return self.at <= max(len(reduce_bits), len(sum_bits))

    stages = Stages()
    grads, input_grads = [], []
    for row in range(row_count):
        row_q, row_k, row_v, row_ctx, row_lse, low, high, bounds = rows[row]
        row_kt = row_k.T
        row_grad = d_context[row * seq_len : (row + 1) * seq_len]
        carried = None
        for part in range(parts):
            staged = row == 0 and stages.busy()
            if row == 0 and part == parts - 1:
                row_grad, output = tie(row_grad, output)
            if row == 0 and part > 0:
                held = (stages.up, stages.down, stages.out, stages.small, stages.piece, term)
                row_grad, held = tie(row_grad, held)
                stages.up, stages.down, stages.out, stages.small, stages.piece, term = held
                input_grads[-1] = lax.psum_scatter(term, "tensor", scatter_dimension=1, tiled=True)
            if staged:
                stages.send()
            final, carried = attend_backward(
                row_q, row_k, row_v, row_kt, row_grad, row_ctx, row_lse, low, high, bounds,
                part, parts, carried,
            )
            if row == 0 and part == 0:
                output, final = tie(output, final)
                output = tokens_to_heads(output)
            if staged:
                stages.moved, final = tie(stages.moved, final)
                stages.add()
            grads.append(final)
            term = inner_last(final[0], w_query) + inner_last(final[1], w_key)
            term = (term + inner_last(final[2], w_value)).reshape(shards, own_len, full_width)
            at = (row * parts + part) * own_len
            mine = lax.broadcasted_iota(jnp.int32, (shards, 1, 1), 0) == me
            term = term + jnp.where(mine, d_first_res[at : at + own_len][None], 0.0)
            term = term.astype(jnp.bfloat16).reshape(part_len, full_width)
            if row > 0 or part == parts - 1:
                term = lax.psum_scatter(term, "tensor", scatter_dimension=1, tiled=True)
            input_grads.append(term)
    while stages.busy():
        stages.send()
        stages.add()
    out_sum, own_sums, own_piece = stages.out, stages.small, stages.piece
    grad_w_out = out_sum.astype(jnp.float32)
    all_pieces = {0: own_piece}
    for bit in first_order + [0]:
        all_pieces = gather_step(all_pieces, bit)
    grad_w_down, grad_w_up = place_pieces([all_pieces[j] for j in range(members)], member)
    sums = [own_sums[i * slice_width : (i + 1) * slice_width] for i in range(6)]
    sum_b_up = own_sums[6 * slice_width : -3]
    totals_all = own_sums[-3:]
    lex_stats = jnp.stack([totals_all[1] / totals_all[0], totals_all[2] / totals_all[0]])

    d_queries, d_keys, d_values = (
        jnp.concatenate([item[i] for item in grads], axis=0) for i in range(3)
    )
    grad_inputs = jnp.concatenate(input_grads, axis=0)
    d_query_sum = sum_members(inner_first(flat, d_queries).astype(jnp.bfloat16), first_order)
    d_key_sum = sum_members(inner_first(flat, d_keys).astype(jnp.bfloat16), second_order)
    d_value_sum = sum_members(inner_first(flat, d_values).astype(jnp.bfloat16), first_order)
    bias_sums = sum_members(
        jnp.stack(
            [
                jnp.sum(d_queries, axis=0, dtype=jnp.float32),
                jnp.sum(d_values, axis=0, dtype=jnp.float32),
            ]
        ),
        first_order,
    )
    out_shape = (row_count, seq_len, slice_width)
    output = output.reshape(shards, row_count * parts, own_len, slice_width)
    output = output.transpose(1, 0, 2, 3)
    return (
        output.reshape(out_shape),
        grad_inputs.reshape(out_shape),
        d_query_sum.astype(jnp.float32),
        bias_sums[0],
        d_key_sum.astype(jnp.float32),
        d_value_sum.astype(jnp.float32),
        bias_sums[1],
        grad_w_out,
        sums[0],
        sums[1],
        sums[2],
        grad_w_up,
        sum_b_up,
        grad_w_down,
        sums[3],
        sums[4],
        sums[5],
        lex_stats,
    )


def solution(mesh):
    in_specs = (
        P("batch", None, None),
        P("batch", None),
        P("batch", None),
        P(None, "tensor"),
        P("tensor"),
        P(None, "tensor"),
        P(None, "tensor"),
        P("tensor"),
        P("tensor", None),
        P("tensor"),
        P("tensor"),
        P("tensor"),
        P(None, "tensor"),
        P("tensor"),
        P("tensor", None),
        P("tensor"),
        P("tensor"),
        P("tensor"),
        P("tensor"),
        P(),
        P("batch", None, "tensor"),
    )
    out_specs = (
        P("batch", None, "tensor"),
        P("batch", None, "tensor"),
        P(None, "tensor"),
        P("tensor"),
        P(None, "tensor"),
        P(None, "tensor"),
        P("tensor"),
        P("tensor", None),
        P("tensor"),
        P("tensor"),
        P("tensor"),
        P(None, "tensor"),
        P("tensor"),
        P("tensor", None),
        P("tensor"),
        P("tensor"),
        P("tensor"),
        P(),
    )
    return jax.shard_map(local, mesh=mesh, in_specs=in_specs, out_specs=out_specs, check_vma=False)
```
